32 devices in a mesh: gx: 2 (over core), gy: 16 (over z, y, x).
Axes of the slice: x: 2, y: 2, z: 4, core: 2. Of those that a mesh axis runs over, the one named last changes fastest.
Arguments:
- data: float32 [32, 256, 128], P('gx', 'gy'), may hold values from -6 to 6
- precond: float32 [32, 256, 128], P('gx', 'gy'), may hold values from 0.5 to 2
- psf: float32 [2, 16, 17, 17, 17], P('gx', 'gy'), may hold values from -0.05 to 0.05
Outputs:
- model: float32 [32, 256, 128], P('gx', 'gy')
- residual: float32 [32, 256, 128], P('gx', 'gy')
The draws below stay inside these ranges and needn't reach their ends.
All inputs are finite; a program needn't handle non-finite values.
Results may differ from the reference program's by a relative error of at most 0.0003.
Values sent between devices are 32-bit elements; how exact they have to be, the bound alone decides.
A program may use at most 64 MiB of HBM per device.

```python
import math
import jax
import jax.numpy as jnp
from jax import lax

CX = 16
CY = 16
NZ = 128
PSF = 17
ITERS = 2
NX = 32
NY = 256
N_GX = 2
N_GY = 16


def block_levels(own_key, dims, pieces, smallest, largest):
    def one(position, shards_of):
        steps = jax.random.uniform(jax.random.fold_in(jax.random.fold_in(own_key, 6), position), (shards_of,), jnp.float32, smallest / len(pieces), largest / len(pieces))
        return jnp.repeat(jnp.exp(steps), dims[position] // shards_of).reshape((-1,) + (1,) * (len(dims) - position - 1))

    loudness = one(*pieces[0])
    for cut in pieces[1:]:
        loudness = loudness * one(*cut)
    return loudness


def centred(stream_key, extent, spread, limit, cuts=(), kind=jnp.bfloat16):
    result = spread * jax.random.normal(stream_key, extent, jnp.float32)
    if cuts:
        result = result * block_levels(stream_key, extent, cuts, -0.22, 0.18)
    return jnp.clip(result, -limit, limit).astype(kind)


def setup_inputs(seed: int = 0) -> dict:
    keys = jax.random.split(jax.random.key(seed), 4)
    return {
        "data": centred(keys[0], (NX, NY, NZ), 1.0, 6.0, ((0, 2), (1, 16)), jnp.float32),
        "precond": jnp.clip(jnp.exp(math.log(2.0) - 1.3862944 * jax.random.uniform(keys[1], (NX, NY, NZ), jnp.float32) ** block_levels(keys[1], (NX, NY, NZ), ((0, 2), (1, 16)), -0.2, 0.2)), 0.5, 2.0),
        "psf": centred(keys[2], (N_GX, N_GY, PSF, PSF, PSF), 0.008, 0.05, ((0, 2), (1, 16)), jnp.float32),
    }


relaxation = 0.7


def node_spectrum(kernel, length_x, length_y, length_z, half):
    width = kernel.shape[0]
    flipped = kernel[::-1, ::-1, ::-1]
    placed = jnp.zeros((length_x, length_y, length_z), kernel.dtype).at[:width, :width, :width].set(flipped)
    return jnp.fft.fftn(jnp.roll(placed, (-half, -half, -half), axis=(0, 1, 2)))


def apply_operator(field, psf):
    width = psf.shape[2]
    half = width // 2
    padded = jnp.pad(field, half)
    length_x = CX + 2 * half
    length_y = CY + 2 * half
    length_z = NZ + 2 * half
    along_x = (jnp.arange(CX, dtype=jnp.float32) + 0.5) / CX
    along_y = (jnp.arange(CY, dtype=jnp.float32) + 0.5) / CY

    def one_tile(index):
        row = (index // N_GY).astype(jnp.int32)
        column = (index % N_GY).astype(jnp.int32)
        row_next = jnp.minimum(row + 1, N_GX - 1).astype(jnp.int32)
        column_next = jnp.minimum(column + 1, N_GY - 1).astype(jnp.int32)
        start = (row * CX).astype(jnp.int32)
        begin = (column * CY).astype(jnp.int32)
        region = lax.dynamic_slice(padded, (start, begin, jnp.int32(0)), (length_x, length_y, length_z))
        region_spectrum = jnp.fft.fftn(region)
        nodes = ((row, column, (1.0 - along_x)[:, None] * (1.0 - along_y)[None, :]),
                 (row_next, column, along_x[:, None] * (1.0 - along_y)[None, :]),
                 (row, column_next, (1.0 - along_x)[:, None] * along_y[None, :]),
                 (row_next, column_next, along_x[:, None] * along_y[None, :]))
        total = jnp.zeros((CX, CY, NZ), field.dtype)
        for node_row, node_column, weight in nodes:
            kernel = psf[node_row, node_column]
            spectrum = node_spectrum(kernel, length_x, length_y, length_z, half)
            full = jnp.real(jnp.fft.ifftn(region_spectrum * spectrum))
            inner = full[half:half + CX, half:half + CY, half:half + NZ]
            total = total + weight[:, :, None].astype(field.dtype) * inner.astype(field.dtype)
        return total

    tiles = lax.map(one_tile, jnp.arange(N_GX * N_GY, dtype=jnp.int32))
    tiles = tiles.reshape(N_GX, N_GY, CX, CY, NZ).transpose(0, 2, 1, 3, 4).reshape(NX, NY, NZ)
    return field + tiles


def reference(data, precond, psf):
    model = precond * data
    residual = data
    for sweep_index in range(ITERS):
        residual = data - apply_operator(model, psf)
        model = model + relaxation * precond * residual
    return model, residual
```

```python
import functools
import math

import jax
import jax.numpy as jnp
import numpy as np
from jax import lax
from jax.experimental import pallas as pl
from jax.experimental.pallas import tpu as pltpu
from jax.sharding import PartitionSpec as P

ITERS = 2
relaxation = 0.7
LANES = 128
SUB = 8
OUTER = 4


def times_phase(value, turn, size, sign):
    if value is None:
        return None
    re, im = value
    turn = (sign * turn) % size
    eighth = 8 * turn
    if eighth == 0:
        return value
    if eighth == 2 * size:
        return (-im, re)
    if eighth == 4 * size:
        return (-re, -im)
    if eighth == 6 * size:
        return (im, -re)
    angle = 2.0 * math.pi * turn / size
    cosine, sine = math.cos(angle), math.sin(angle)
    if eighth % size == 0:
        root = math.sqrt(0.5)
        first, second = (re - im) * root, (re + im) * root
        if eighth == size:
            return (first, second)
        if eighth == 3 * size:
            return (-second, first)
        if eighth == 5 * size:
            return (-first, -second)
        return (second, -first)
    return (re * cosine - im * sine, re * sine + im * cosine)


def plus(a, b):
    if a is None:
        return b
    if b is None:
        return a
    return (a[0] + b[0], a[1] + b[1])


def minus(a, b):
    if b is None:
        return a
    if a is None:
        return (-b[0], -b[1])
    return (a[0] - b[0], a[1] - b[1])


def transform(values, sign, wanted):
    size = len(values)
    if all(v is None for v in values):
        return [None] * wanted
    if size == 1:
        return list(values)
    half = size // 2
    if size % 2:
        raise ValueError("length")
    even = transform(values[0::2], sign, min(half, wanted))
    odd = transform(values[1::2], sign, min(half, wanted))
    odd = [times_phase(v, k, size, sign) for k, v in enumerate(odd)]
    low = [plus(a, b) for a, b in zip(even, odd)]
    high = [minus(a, b) for a, b in zip(even, odd)]
    return (low + high)[:wanted]


def tables(depth, width):
    half = width // 2
    length = depth + 2 * half
    count = length // 2 + 1
    k = np.arange(count)
    field = np.zeros((depth, 2 * LANES))
    turns = (np.arange(depth)[:, None] + half) * k[None, :] % length
    angle = turns * (2.0 * np.pi / length)
    field[:, :count] = np.cos(angle)
    field[:, LANES : LANES + count] = -np.sin(angle)
    kernel = np.zeros((LANES, 2 * LANES))
    angle = np.arange(width)[:, None] * k[None, :] % length * (2.0 * np.pi / length)
    kernel[:width, :count] = np.cos(angle)
    kernel[:width, LANES : LANES + count] = np.sin(angle)
    back = np.zeros((2 * LANES, depth))
    weight = np.where((k == 0) | (2 * k == length), 1.0, 2.0) / length
    angle = k[:, None] * np.arange(depth)[None, :] % length * (2.0 * np.pi / length)
    back[:count] = weight[:, None] * np.cos(angle)
    back[LANES : LANES + count] = -weight[:, None] * np.sin(angle)
    return field, kernel, back


def stacked(table):
    high = jnp.asarray(table, jnp.float32).astype(jnp.bfloat16)
    low = (jnp.asarray(table, jnp.float32) - high.astype(jnp.float32)).astype(jnp.bfloat16)
    return jnp.concatenate([high, high, low])


def product(left, table):
    high = left.astype(jnp.bfloat16)
    low = (left - high.astype(jnp.float32)).astype(jnp.bfloat16)
    left = jnp.concatenate([high, low, high], axis=1)
    return jnp.dot(left, table, preferred_element_type=jnp.float32)


def first_pass(load, keep, size, sign):
    inner = size // OUTER
    for r in range(OUTER):
        values = transform([load(OUTER * a + r) for a in range(inner)], sign, inner)
        for m, value in enumerate(values):
            keep(r * inner + m, times_phase(value, r * m, size, sign))


def second_pass(kept, size, sign, wanted):
    inner = size // OUTER
    for m in range(inner):
        values = [kept(r * inner + m) for r in range(OUTER)]
        for q, value in enumerate(transform(values, sign, wanted // inner)):
            yield m + inner * q, value


def keeper(buffer, slot):
    def keep(n, value):
        buffer[slot, 0, n], buffer[slot, 1, n] = value

    def kept(n):
        return buffer[slot, 0, n], buffer[slot, 1, n]

    return keep, kept


def spectra(width, region_x, region_y, rows, first, packed, table_ref, g_ref, k1, k2, work):
    per = LANES // width
    full = width - 1
    for a in range(width):
        shifted = packed[a // per]
        if a % per:
            shifted = pltpu.roll(shifted, LANES - width * (a % per), axis=1)
        both = product(shifted, table_ref[...])
        k1[0, pl.ds(a * rows, rows), :] = both[:, :LANES]
        k1[1, pl.ds(a * rows, rows), :] = both[:, LANES:]

    @pl.loop(0, rows // SUB)
    def _(tile):
        at = lambda i: pl.ds(pl.multiple_of(i * rows + tile * SUB, SUB), SUB)
        load = lambda a: (k1[0, at(a), :], k1[1, at(a), :]) if a < width else None
        keep, kept = keeper(work, 0)
        first_pass(load, keep, region_x, 1)
        for kx, (re, im) in second_pass(kept, region_x, 1, region_x):
            k2[0, at(kx), :] = re
            k2[1, at(kx), :] = im

    @pl.loop(0, 2)
    def _(node):
        @pl.loop(0, region_x // SUB)
        def _(tile):
            def load(b):
                if b >= width:
                    return None
                row = node * full + b if b < full else 2 * full + node
                at = pl.ds(tile * SUB * rows + row, SUB, stride=rows)
                return k2[0, at, :], k2[1, at, :]

            keep, kept = keeper(work, 0)
            first_pass(load, keep, region_y, 1)
            for ky, (re, im) in second_pass(kept, region_y, 1, region_y):
                to = pl.ds(pl.multiple_of(ky * region_x + tile * SUB, SUB), SUB)
                g_ref[first + node, 0, to, :] = re
                g_ref[first + node, 1, to, :] = im


def depth_forward(region, box, field_ref, z):
    x0, nx, y0, ny = box
    region_y = region.shape[1]
    step = max(1, 2 * LANES // ny)
    for x in range(x0, x0 + nx, step):
        count = min(step, x0 + nx - x)
        left = region[pl.ds(x, count), pl.ds(y0, ny), :].reshape(count * ny, LANES)
        both = product(left, field_ref[...])
        for i in range(count):
            to = pl.ds((x + i) * region_y + y0, ny)
            z[0, to, :] = both[i * ny : (i + 1) * ny, :LANES]
            z[1, to, :] = both[i * ny : (i + 1) * ny, LANES:]


def inline_forward(tile, region_x, region_y, pitch, z, c, work):
    def load(x):
        at = pl.ds(pl.multiple_of(x * region_y + tile * SUB, SUB), SUB)
        return z[0, at, :], z[1, at, :]

    keep, kept = keeper(work, 0)
    first_pass(load, keep, region_x, -1)
    for kx, (re, im) in second_pass(kept, region_x, -1, region_x):
        to = pl.ds(pl.multiple_of(kx * pitch + tile * SUB, SUB), SUB)
        c[0, to, :] = re
        c[1, to, :] = im


def crossline(count_y, region_x, region_y, pitch, g_ref, c, v, u, work):
    @pl.loop(0, region_x // SUB)
    def _(tile):
        def load(y):
            at = pl.ds(tile * SUB * pitch + y, SUB, stride=pitch)
            return c[0, at, :], c[1, at, :]

        keep, kept = keeper(work, 0)
        first_pass(load, keep, region_y, -1)
        for ky, (re, im) in second_pass(kept, region_y, -1, region_y):
            v[0, ky] = re
            v[1, ky] = im

        @pl.loop(0, 2)
        def _(i):
            for j in range(2):
                def load(ky):
                    at = pl.ds(pl.multiple_of(ky * region_x + tile * SUB, SUB), SUB)
                    gr, gi = g_ref[2 * j + i, 0, at, :], g_ref[2 * j + i, 1, at, :]
                    vr, vi = v[0, ky], v[1, ky]
                    return vr * gr - vi * gi, vr * gi + vi * gr

                keep, _ = keeper(work, j)
                first_pass(load, keep, region_y, 1)
            passes = [second_pass(keeper(work, j)[1], region_y, 1, count_y) for j in range(2)]
            for (y, (ar, ai)), (_, (br, bi)) in zip(*passes):
                t = (y + 0.5) / count_y
                to = pl.ds(pl.multiple_of(y * pitch + tile * SUB, SUB), SUB)
                u[i, 0, to, :] = (1.0 - t) * ar + t * br
                u[i, 1, to, :] = (1.0 - t) * ai + t * bi


def inline_back(tile, count_x, region_x, pitch, u, w, work):
    for i in range(2):
        def load(kx):
            at = pl.ds(tile * SUB * pitch + kx, SUB, stride=pitch)
            return u[i, 0, at, :], u[i, 1, at, :]

        keep, _ = keeper(work, i)
        first_pass(load, keep, region_x, 1)
    passes = [second_pass(keeper(work, i)[1], region_x, 1, count_x) for i in range(2)]
    for (x, (ar, ai)), (_, (br, bi)) in zip(*passes):
        s = (x + 0.5) / count_x
        w[tile, pl.ds(x * SUB, SUB), :LANES] = (1.0 - s) * ar + s * br
        w[tile, pl.ds(x * SUB, SUB), LANES:] = (1.0 - s) * ai + s * bi


class Link:
    def __init__(self, sems, k, src, dst, axis, by, only=True):
        here, size = lax.axis_index(axis), lax.axis_size(axis)
        inside = lambda i: jnp.logical_and(jnp.logical_and(i >= 0, i < size), only)
        self.sends, self.gets = inside(here + by), inside(here - by)
        self.copy = pltpu.make_async_remote_copy(
            src_ref=src, dst_ref=dst, send_sem=sems[0].at[k], recv_sem=sems[1].at[k],
            device_id={axis: here + by}, device_id_type=pl.DeviceIdType.MESH,
        )

    def start(self):
        pl.when(self.sends)(lambda: self.copy.start())

    def wait_recv(self):
        pl.when(self.gets)(lambda: self.copy.wait_recv())

    def wait_send(self):
        pl.when(self.sends)(lambda: self.copy.wait_send())


LINKS = 10


def halo_links(region, count_x, count_y, half, sems, base):
    gy, size = lax.axis_index("gy"), lax.axis_size("gy")
    own_x = pl.ds(half, count_x)
    low, high_x, high_y = pl.ds(0, half), pl.ds(half + count_x, half), pl.ds(half + count_y, half)
    last_x, last_y, first = pl.ds(count_x, half), pl.ds(count_y, half), pl.ds(half, half)
    at = lambda x, y: region.at[x, y]
    along_y = [
        Link(sems, base, at(own_x, first), at(own_x, high_y), "gy", -1),
        Link(sems, base + 1, at(own_x, last_y), at(own_x, low), "gy", 1),
    ]
    along_x = []
    for n in range(2):
        part = pl.ds(half + n * (count_y // 2), count_y // 2)
        along_x.append([
            Link(sems, base + 2 + 2 * n, at(last_x, part), at(low, part), "gx", 1),
            Link(sems, base + 3 + 2 * n, at(first, part), at(high_x, part), "gx", -1),
        ])
    relayed = [
        [
            Link(sems, base + 6, at(last_x, high_y), at(low, high_y), "gx", 1, gy < size - 1),
            Link(sems, base + 7, at(first, high_y), at(high_x, high_y), "gx", -1, gy < size - 1),
        ],
        [
            Link(sems, base + 8, at(last_x, low), at(low, low), "gx", 1, gy > 0),
            Link(sems, base + 9, at(first, low), at(high_x, low), "gx", -1, gy > 0),
        ],
    ]
    return along_y, along_x, relayed


def whole_kernel(
    count_x, count_y, half, rows, pitch,
    data_hbm, precond_hbm, psf_hbm, field_hbm, kernel_hbm, back_hbm,
    model_ref, residual_ref,
    data_ref, precond_ref, psf_ref, field_ref, kernel_ref, back_ref,
    region0, region1, wide, nodes, packed, g_ref, k1, k2, z, c, v, u, w, work,
    load_sem, send_sem, recv_sem,
):
    width = 2 * half + 1
    full = width - 1
    per = LANES // width
    region_x, region_y = count_x + 2 * half, count_y + 2 * half
    sems = (send_sem, recv_sem)
    gx, gy = lax.axis_index("gx"), lax.axis_index("gy")
    size_x, size_y = lax.axis_size("gx"), lax.axis_size("gy")
    regions = [region0, region1]

    barrier = pltpu.get_barrier_semaphore()
    for axis, here, size in (("gx", gx, size_x), ("gy", gy, size_y)):
        for by in (-1, 1):
            @pl.when(jnp.logical_and(here + by >= 0, here + by < size))
            def _():
                pl.semaphore_signal(
                    barrier, inc=1, device_id={axis: here + by},
                    device_id_type=pl.DeviceIdType.MESH,
                )

    pairs = [
        (psf_hbm.at[:, :, 0, :], psf_ref), (data_hbm, data_ref), (precond_hbm, precond_ref),
        (kernel_hbm, kernel_ref), (field_hbm, field_ref), (back_hbm, back_ref),
    ]
    loads = [pltpu.make_async_copy(a, b, load_sem.at[k]) for k, (a, b) in enumerate(pairs)]
    for load in loads:
        load.start()

    wide[...] = jnp.zeros(wide.shape, wide.dtype)
    packed[...] = jnp.zeros(packed.shape, packed.dtype)
    every = slice(None)
    edges = [
        (gx == 0, (pl.ds(0, half), every)), (gx == size_x - 1, (pl.ds(half + count_x, half), every)),
        (gy == 0, (every, pl.ds(0, half))), (gy == size_y - 1, (every, pl.ds(half + count_y, half))),
    ]
    for edge, at in edges:
        @pl.when(edge)
        def _():
            for region in regions:
                region[at] = jnp.zeros(region[at].shape, region.dtype)

    loads[0].wait()
    for a in range(width):
        wide[a, pl.ds(0, width), pl.ds(0, width)] = psf_ref[a]
    for n in range(nodes.shape[1]):
        total = wide[n * per]
        for a in range(n * per + 1, min(width, (n + 1) * per)):
            total = total + pltpu.roll(wide[a], width * (a % per), axis=1)
        nodes[0, n] = total
    loads[1].wait()
    loads[2].wait()
    own = (pl.ds(half, count_x), pl.ds(half, count_y))
    region0[own] = precond_ref[...] * data_ref[...]

    peers = 0
    for here, size in ((gx, size_x), (gy, size_y)):
        peers += (here > 0).astype(jnp.int32) + (here < size - 1).astype(jnp.int32)
    pl.semaphore_wait(barrier, peers)

    inline = Link(sems, 0, nodes.at[0], nodes.at[1], "gx", -1)
    cross = Link(sems, 1, nodes.at[0], nodes.at[2], "gy", -1)
    corner = Link(sems, 2, nodes.at[2], nodes.at[3], "gx", -1, gy < size_y - 1)
    cross.start()
    inline.start()
    started = [cross, inline, corner]
    last_x, last_y = gx == size_x - 1, gy == size_y - 1

    def pack(place, node):
        at = pl.ds(place * full, full)
        packed[:, at, :] = nodes[node, :, pl.ds(0, full), :]
        packed[:, pl.ds(2 * full + place, 1), :] = nodes[node, :, pl.ds(full, 1), :]

    def pair_spectra(first):
        spectra(
            width, region_x, region_y, rows, first, packed, kernel_ref, g_ref, k1, k2, work
        )

    links = [
        halo_links(regions[n], count_x, count_y, half, sems, 3 + LINKS * n) for n in range(ITERS)
    ]
    for sweep_index in range(ITERS):
        region = regions[sweep_index]
        along_y, along_x, relayed = links[sweep_index]
        started += along_y + along_x[0] + along_x[1] + relayed[0] + relayed[1]
        if sweep_index == 0:
            for link in along_x[0] + along_x[1] + along_y:
                link.start()
            loads[3].wait()
            pack(0, 0)
            inline.wait_recv()
            pl.when(last_x)(lambda: pack(1, 0))
            pl.when(jnp.logical_not(last_x))(lambda: pack(1, 1))
            pair_spectra(0)
            cross.wait_recv()
            corner.start()
            loads[4].wait()
        depth_forward(region, (half, count_x, half, count_y), field_ref, z)
        for link in along_x[0] + along_x[1]:
            link.wait_recv()
        depth_forward(region, (0, half, half, count_y), field_ref, z)
        depth_forward(region, (half + count_x, half, half, count_y), field_ref, z)

        @pl.loop(half // SUB, (half + count_y) // SUB)
        def _(tile):
            inline_forward(tile, region_x, region_y, pitch, z, c, work)

        if sweep_index == 0:
            corner.wait_recv()
            pl.when(last_y)(lambda: pack(0, 0))
            pl.when(jnp.logical_not(last_y))(lambda: pack(0, 2))
            for edge_x in (False, True):
                for edge_y in (False, True):
                    here = (last_x if edge_x else jnp.logical_not(last_x),
                            last_y if edge_y else jnp.logical_not(last_y))
                    source = (0 if edge_y else 2) if edge_x else (1 if edge_y else 3)
                    pl.when(jnp.logical_and(*here))(lambda: pack(1, source))
            pair_spectra(2)
        for n in range(2):
            along_y[n].wait_recv()
            for link in relayed[n]:
                link.start()
        depth_forward(region, (half, count_x, 0, half), field_ref, z)
        depth_forward(region, (half, count_x, half + count_y, half), field_ref, z)
        for link in relayed[0] + relayed[1]:
            link.wait_recv()
        for x0 in (0, half + count_x):
            for y0 in (0, half + count_y):
                depth_forward(region, (x0, half, y0, half), field_ref, z)

        @pl.loop(0, 2)
        def _(n):
            @pl.loop(0, half // SUB)
            def _(tile):
                at = n * ((half + count_y) // SUB) + tile
                inline_forward(at, region_x, region_y, pitch, z, c, work)

        crossline(count_y, region_x, region_y, pitch, g_ref, c, v, u, work)
        last = sweep_index == ITERS - 1
        if sweep_index == 0:
            loads[5].wait()
        for tile in range(count_y // SUB):
            inline_back(tile, count_x, region_x, pitch, u, w, work)
            blended = product(w[tile], back_ref[...])
            here = pl.ds(tile * SUB, SUB)
            inner = pl.ds(half + tile * SUB, SUB)
            for x in range(count_x):
                model = region[x + half, inner, :]
                residual = data_ref[x, here, :] - (model + blended[x * SUB : (x + 1) * SUB])
                model = model + relaxation * precond_ref[x, here, :] * residual
                if last:
                    residual_ref[x, here, :] = residual
                    model_ref[x, here, :] = model
                else:
                    regions[sweep_index + 1][x + half, inner, :] = model
            if not last:
                per_half = count_y // SUB // 2
                if (tile + 1) % per_half == 0:
                    n = (tile + 1) // per_half - 1
                    after_y, after_x, _ = links[sweep_index + 1]
                    for link in [after_y[n]] + after_x[n]:
                        link.start()
    for link in started:
        link.wait_send()


def local(data, precond, psf):
    count_x, count_y, depth = data.shape
    width = psf.shape[2]
    half = width // 2
    region_x, region_y = count_x + 2 * half, count_y + 2 * half
    field, kernel, back = tables(depth, width)
    back = back / (region_x * region_y)
    f32 = jnp.float32
    up = lambda n, m: -(-n // m) * m
    high, columns = up(width, SUB), up(width, LANES // width) // (LANES // width)
    rows = up(2 * width, SUB)
    pitch = max(region_x, region_y) + SUB
    vmem = lambda *shape: pltpu.VMEM(shape, f32)
    table = lambda *shape: pltpu.VMEM(shape, jnp.bfloat16)
    square = region_x * region_y
    flat = psf.transpose(0, 2, 3, 1, 4).reshape(width, width, 1, width)
    operands = (data, precond, flat, stacked(field), stacked(kernel), stacked(back))
    model, residual = pl.pallas_call(
        functools.partial(whole_kernel, count_x, count_y, half, rows, pitch),
        out_shape=[jax.ShapeDtypeStruct(data.shape, f32)] * 2,
        in_specs=[pl.BlockSpec(memory_space=pltpu.HBM)] * 6,
        out_specs=[pl.BlockSpec(memory_space=pltpu.VMEM)] * 2,
        scratch_shapes=[
            vmem(*data.shape),
            vmem(*data.shape),
            vmem(width, width, width),
            table(*operands[3].shape),
            table(*operands[4].shape),
            table(*operands[5].shape),
            vmem(region_x, region_y, depth),
            vmem(region_x, region_y, depth),
            vmem(width, high, LANES),
            vmem(4, columns, high, LANES),
            vmem(columns, rows, LANES),
            vmem(4, 2, square, LANES),
            vmem(2, width * rows, LANES),
            vmem(2, region_x * rows, LANES),
            vmem(2, square, LANES),
            vmem(2, region_x * pitch, LANES),
            vmem(2, region_y, SUB, LANES),
            vmem(2, 2, count_y * pitch, LANES),
            vmem(count_y // SUB, count_x * SUB, 2 * LANES),
            vmem(2, 2, max(region_x, region_y), SUB, LANES),
            pltpu.SemaphoreType.DMA((6,)),
            pltpu.SemaphoreType.DMA((3 + LINKS * ITERS,)),
            pltpu.SemaphoreType.DMA((3 + LINKS * ITERS,)),
        ],
        compiler_params=pltpu.CompilerParams(
            vmem_limit_bytes=54976 << 10, collective_id=0, has_side_effects=True
        ),
        name="whole",
    )(*operands)
    def tail(a, b, c, e, sems):
        copies = [pltpu.make_async_copy(a, c, sems.at[0]), pltpu.make_async_copy(b, e, sems.at[1])]
        for copy in copies:
            copy.start()
        for copy in copies:
            copy.wait()

    return pl.pallas_call(
        tail,
        out_shape=[jax.ShapeDtypeStruct(data.shape, f32)] * 2,
        in_specs=[pl.BlockSpec(memory_space=pltpu.VMEM)] * 2,
        out_specs=[pl.BlockSpec(memory_space=pl.ANY)] * 2,
        scratch_shapes=[pltpu.SemaphoreType.DMA((2,))],
        compiler_params=pltpu.CompilerParams(vmem_limit_bytes=54976 << 10),
        name="tail",
    )(model, residual)


def solution(mesh):
    placed = (P("gx", "gy", None), P("gx", "gy", None), P("gx", "gy", None, None, None))
    return jax.shard_map(
        local,
        mesh=mesh,
        in_specs=placed,
        out_specs=(P("gx", "gy", None), P("gx", "gy", None)),
        check_vma=False,
    )
```

```python
import functools
import math

import jax
import jax.numpy as jnp
import numpy as np
from jax import lax
from jax.experimental import pallas as pl
from jax.experimental.pallas import tpu as pltpu
from jax.sharding import PartitionSpec as P

ITERS = 2
relaxation = 0.7
LANES = 128
SUB = 8
OUTER = 4


def times_phase(value, turn, size, sign):
    if value is None:
        return None
    re, im = value
    turn = (sign * turn) % size
    eighth = 8 * turn
    if eighth == 0:
        return value
    if eighth == 2 * size:
        return (-im, re)
    if eighth == 4 * size:
        return (-re, -im)
    if eighth == 6 * size:
        return (im, -re)
    angle = 2.0 * math.pi * turn / size
    cosine, sine = math.cos(angle), math.sin(angle)
    if eighth % size == 0:
        root = math.sqrt(0.5)
        first, second = (re - im) * root, (re + im) * root
        if eighth == size:
            return (first, second)
        if eighth == 3 * size:
            return (-second, first)
        if eighth == 5 * size:
            return (-first, -second)
        return (second, -first)
    return (re * cosine - im * sine, re * sine + im * cosine)


def plus(a, b):
    if a is None:
        return b
    if b is None:
        return a
    return (a[0] + b[0], a[1] + b[1])


def minus(a, b):
    if b is None:
        return a
    if a is None:
        return (-b[0], -b[1])
    return (a[0] - b[0], a[1] - b[1])


def transform(values, sign, wanted):
    size = len(values)
    if all(v is None for v in values):
        return [None] * wanted
    if size == 1:
        return list(values)
    half = size // 2
    if size % 2:
        raise ValueError("length")
    even = transform(values[0::2], sign, min(half, wanted))
    odd = transform(values[1::2], sign, min(half, wanted))
    odd = [times_phase(v, k, size, sign) for k, v in enumerate(odd)]
    low = [plus(a, b) for a, b in zip(even, odd)]
    high = [minus(a, b) for a, b in zip(even, odd)]
    return (low + high)[:wanted]


def tables(depth, width):
    half = width // 2
    length = depth + 2 * half
    count = length // 2 + 1
    k = np.arange(count)
    field = np.zeros((depth, 2 * LANES))
    turns = (np.arange(depth)[:, None] + half) * k[None, :] % length
    angle = turns * (2.0 * np.pi / length)
    field[:, :count] = np.cos(angle)
    field[:, LANES : LANES + count] = -np.sin(angle)
    kernel = np.zeros((LANES, 2 * LANES))
    angle = np.arange(width)[:, None] * k[None, :] % length * (2.0 * np.pi / length)
    kernel[:width, :count] = np.cos(angle)
    kernel[:width, LANES : LANES + count] = np.sin(angle)
    back = np.zeros((2 * LANES, depth))
    weight = np.where((k == 0) | (2 * k == length), 1.0, 2.0) / length
    angle = k[:, None] * np.arange(depth)[None, :] % length * (2.0 * np.pi / length)
    back[:count] = weight[:, None] * np.cos(angle)
    back[LANES : LANES + count] = -weight[:, None] * np.sin(angle)
    return field, kernel, back


def stacked(table):
    high = jnp.asarray(table, jnp.float32).astype(jnp.bfloat16)
    low = (jnp.asarray(table, jnp.float32) - high.astype(jnp.float32)).astype(jnp.bfloat16)
    return jnp.concatenate([high, high, low])


def product(left, table):
    high = left.astype(jnp.bfloat16)
    low = (left - high.astype(jnp.float32)).astype(jnp.bfloat16)
    left = jnp.concatenate([high, low, high], axis=1)
    return jnp.dot(left, table, preferred_element_type=jnp.float32)


def first_pass(load, keep, size, sign):
    inner = size // OUTER
    for r in range(OUTER):
        values = transform([load(OUTER * a + r) for a in range(inner)], sign, inner)
        for m, value in enumerate(values):
            keep(r * inner + m, times_phase(value, r * m, size, sign))


def second_pass(kept, size, sign, wanted):
    inner = size // OUTER
    for m in range(inner):
        values = [kept(r * inner + m) for r in range(OUTER)]
        for q, value in enumerate(transform(values, sign, wanted // inner)):
            yield m + inner * q, value


def keeper(buffer, slot):
    def keep(n, value):
        buffer[slot, 0, n], buffer[slot, 1, n] = value

    def kept(n):
        return buffer[slot, 0, n], buffer[slot, 1, n]

    return keep, kept


def rows_of(count, width):
    return -(-count * width // SUB) * SUB


def row_of(count, width, node, b):
    full = width - 1
    return node * full + b if b < full else count * full + node


def spectra(count, width, region_x, region_y, first, packed, table_ref, g_ref, k1, k2, left, work):
    per, rows = LANES // width, rows_of(count, width)
    for a in range(width):
        shifted = packed[a // per, pl.ds(0, rows), :]
        if a % per:
            shifted = pltpu.roll(shifted, LANES - width * (a % per), axis=1)
        left[pl.ds(a * rows, rows), :] = shifted
    both = product(left[pl.ds(0, width * rows), :], table_ref[...])
    k1[0, pl.ds(0, width * rows), :] = both[:, :LANES]
    k1[1, pl.ds(0, width * rows), :] = both[:, LANES:]

    @pl.loop(0, rows // SUB)
    def _(tile):
        at = lambda i: pl.ds(pl.multiple_of(i * rows + tile * SUB, SUB), SUB)
        load = lambda a: (k1[0, at(a), :], k1[1, at(a), :]) if a < width else None
        keep, kept = keeper(work, 0)
        first_pass(load, keep, region_x, 1)
        for kx, (re, im) in second_pass(kept, region_x, 1, region_x):
            k2[0, at(kx), :] = re
            k2[1, at(kx), :] = im

    for node in range(count):
        @pl.loop(0, region_x // SUB)
        def _(tile):
            def load(b):
                if b >= width:
                    return None
                row = row_of(count, width, node, b)
                at = pl.ds(tile * SUB * rows + row, SUB, stride=rows)
                return k2[0, at, :], k2[1, at, :]

            keep, kept = keeper(work, 0)
            first_pass(load, keep, region_y, 1)
            for ky, (re, im) in second_pass(kept, region_y, 1, region_y):
                to = pl.ds(pl.multiple_of(ky * region_x + tile * SUB, SUB), SUB)
                g_ref[first + node, 0, to, :] = re
                g_ref[first + node, 1, to, :] = im


def halo_terms(half, count_y):
    terms = []
    for y in range(half):
        terms += [(y, y + b, b) for b in range(half - y)]
    for y in range(count_y - half, count_y):
        first = half + count_y
        terms += [(y, n, n - y) for n in range(first, y + 2 * half + 1)]
    return terms


def blend_kernels(half, count_x, count_y, places, kb):
    region_x, region_y = count_x + 2 * half, count_y + 2 * half
    width = 2 * half + 1
    terms = halo_terms(half, count_y)

    @pl.loop(0, region_x // SUB)
    def _(tile):
        for i in range(2):
            def kernel(j, b):
                ref, count, node = places[2 * j + i]
                rows = rows_of(count, width)
                at = pl.ds(tile * SUB * rows + row_of(count, width, node, b), SUB, stride=rows)
                return ref[0, at, :], ref[1, at, :]

            for b in range(width):
                mine = [(n, y) for n, (y, _, lag) in enumerate(terms) if lag == b]
                if not mine:
                    continue
                (ar, ai), (br, bi) = kernel(0, b), kernel(1, b)
                for n, y in mine:
                    t = (y + 0.5) / count_y
                    low, high = region_y * (1.0 - t), region_y * t
                    kb[i, tile, n, 0] = low * ar + high * br
                    kb[i, tile, n, 1] = low * ai + high * bi


def add_halo(half, count_x, count_y, pitch, c, kb, u):
    region_x, region_y = count_x + 2 * half, count_y + 2 * half
    terms = list(enumerate(halo_terms(half, count_y)))

    @pl.loop(0, region_x // SUB)
    def _(tile):
        for side in (range(half), range(half + count_y, region_y)):
            halo = {}
            for n in side:
                at = pl.ds(tile * SUB * pitch + n, SUB, stride=pitch)
                halo[n] = c[0, at, :], c[1, at, :]
            for i in range(2):
                for y in range(count_y):
                    mine = [(k, n) for k, (to, n, _) in terms if to == y and n in halo]
                    if not mine:
                        continue
                    at = pl.ds(pl.multiple_of(y * pitch + tile * SUB, SUB), SUB)
                    re, im = u[i, 0, at, :], u[i, 1, at, :]
                    for k, n in mine:
                        kr, ki = kb[i, tile, k, 0], kb[i, tile, k, 1]
                        vr, vi = halo[n]
                        re = re + (vr * kr - vi * ki)
                        im = im + (vr * ki + vi * kr)
                    u[i, 0, at, :] = re
                    u[i, 1, at, :] = im


def depth_forward(region, box, field_ref, z):
    x0, nx, y0, ny = box
    region_y = region.shape[1]
    step = max(1, 2 * LANES // ny)
    for x in range(x0, x0 + nx, step):
        count = min(step, x0 + nx - x)
        left = region[pl.ds(x, count), pl.ds(y0, ny), :].reshape(count * ny, LANES)
        both = product(left, field_ref[...])
        for i in range(count):
            to = pl.ds((x + i) * region_y + y0, ny)
            z[0, to, :] = both[i * ny : (i + 1) * ny, :LANES]
            z[1, to, :] = both[i * ny : (i + 1) * ny, LANES:]


def inline_forward(tile, region_x, region_y, pitch, z, c, work):
    def load(x):
        at = pl.ds(pl.multiple_of(x * region_y + tile * SUB, SUB), SUB)
        return z[0, at, :], z[1, at, :]

    keep, kept = keeper(work, 0)
    first_pass(load, keep, region_x, -1)
    for kx, (re, im) in second_pass(kept, region_x, -1, region_x):
        to = pl.ds(pl.multiple_of(kx * pitch + tile * SUB, SUB), SUB)
        c[0, to, :] = re
        c[1, to, :] = im


def crossline(present, count_y, region_x, region_y, pitch, g_ref, c, v, u, work):
    @pl.loop(0, region_x // SUB)
    def _(tile):
        def load(y):
            if y not in present:
                return None
            at = pl.ds(tile * SUB * pitch + y, SUB, stride=pitch)
            return c[0, at, :], c[1, at, :]

        keep, kept = keeper(work, 0)
        first_pass(load, keep, region_y, -1)
        for ky, (re, im) in second_pass(kept, region_y, -1, region_y):
            v[0, ky] = re
            v[1, ky] = im

        @pl.loop(0, 2)
        def _(i):
            for j in range(2):
                def load(ky):
                    at = pl.ds(pl.multiple_of(ky * region_x + tile * SUB, SUB), SUB)
                    gr, gi = g_ref[2 * j + i, 0, at, :], g_ref[2 * j + i, 1, at, :]
                    vr, vi = v[0, ky], v[1, ky]
                    return vr * gr - vi * gi, vr * gi + vi * gr

                keep, _ = keeper(work, j)
                first_pass(load, keep, region_y, 1)
            passes = [second_pass(keeper(work, j)[1], region_y, 1, count_y) for j in range(2)]
            for (y, (ar, ai)), (_, (br, bi)) in zip(*passes):
                t = (y + 0.5) / count_y
                to = pl.ds(pl.multiple_of(y * pitch + tile * SUB, SUB), SUB)
                u[i, 0, to, :] = (1.0 - t) * ar + t * br
                u[i, 1, to, :] = (1.0 - t) * ai + t * bi


def inline_back(tile, count_x, region_x, pitch, u, w, work):
    for i in range(2):
        def load(kx):
            at = pl.ds(tile * SUB * pitch + kx, SUB, stride=pitch)
            return u[i, 0, at, :], u[i, 1, at, :]

        keep, _ = keeper(work, i)
        first_pass(load, keep, region_x, 1)
    passes = [second_pass(keeper(work, i)[1], region_x, 1, count_x) for i in range(2)]
    for (x, (ar, ai)), (_, (br, bi)) in zip(*passes):
        s = (x + 0.5) / count_x
        w[tile, pl.ds(x * SUB, SUB), :LANES] = (1.0 - s) * ar + s * br
        w[tile, pl.ds(x * SUB, SUB), LANES:] = (1.0 - s) * ai + s * bi


class Link:
    def __init__(self, sems, k, src, dst, axis, by, only=True):
        here, size = lax.axis_index(axis), lax.axis_size(axis)
        inside = lambda i: jnp.logical_and(jnp.logical_and(i >= 0, i < size), only)
        self.sends, self.gets = inside(here + by), inside(here - by)
        self.copy = pltpu.make_async_remote_copy(
            src_ref=src, dst_ref=dst, send_sem=sems[0].at[k], recv_sem=sems[1].at[k],
            device_id={axis: here + by}, device_id_type=pl.DeviceIdType.MESH,
        )

    def start(self):
        pl.when(self.sends)(lambda: self.copy.start())

    def wait_recv(self):
        pl.when(self.gets)(lambda: self.copy.wait_recv())

    def wait_send(self):
        pl.when(self.sends)(lambda: self.copy.wait_send())


LINKS = 12


def halo_links(region, count_x, count_y, half, sems, base):
    gx, gy, size = lax.axis_index("gx"), lax.axis_index("gy"), lax.axis_size("gy")
    low, high_x, high_y = pl.ds(0, half), pl.ds(half + count_x, half), pl.ds(half + count_y, half)
    last_x, last_y, first = pl.ds(count_x, half), pl.ds(count_y, half), pl.ds(half, half)
    at = lambda x, y: region.at[x, y]
    part_x, part_y = count_x // 2, count_y // 2
    along_y = []
    for n, (src, dst, by) in enumerate(((first, high_y, -1), (last_y, low, 1))):
        along_y.append([])
        for k in range(2):
            x = pl.ds(half + part_x * ((gx + 1 + k) % 2), part_x)
            along_y[n].append(Link(sems, base + 2 * n + k, at(x, src), at(x, dst), "gy", by))
    along_x = []
    for n in range(2):
        part = pl.ds(half + n * part_y, part_y)
        along_x.append([
            Link(sems, base + 4 + 2 * n, at(last_x, part), at(low, part), "gx", 1),
            Link(sems, base + 5 + 2 * n, at(first, part), at(high_x, part), "gx", -1),
        ])
    relayed = []
    for n, (y, has) in enumerate(((high_y, gy < size - 1), (low, gy > 0))):
        relayed.append([
            Link(sems, base + 8 + 2 * n, at(last_x, y), at(low, y), "gx", 1, has),
            Link(sems, base + 9 + 2 * n, at(first, y), at(high_x, y), "gx", -1, has),
        ])
    return along_y, along_x, relayed


def whole_kernel(
    count_x, count_y, half, pitch,
    data_hbm, precond_hbm, psf_hbm, field_hbm, kernel_hbm, back_hbm,
    model_ref, residual_ref,
    data_ref, precond_ref, psf_ref, field_ref, kernel_ref, back_ref,
    region0, region1, wide, nodes, packed, left, g_ref, k1, k2a, k2b, k2c, kb, z, c, v, u, w, work,
    load_sem, send_sem, recv_sem,
):
    width = 2 * half + 1
    full = width - 1
    per = LANES // width
    region_x, region_y = count_x + 2 * half, count_y + 2 * half
    sems = (send_sem, recv_sem)
    gx, gy = lax.axis_index("gx"), lax.axis_index("gy")
    size_x, size_y = lax.axis_size("gx"), lax.axis_size("gy")
    regions = [region0, region1]

    barrier = pltpu.get_barrier_semaphore()
    for axis, here, size in (("gx", gx, size_x), ("gy", gy, size_y)):
        for by in (-1, 1):
            @pl.when(jnp.logical_and(here + by >= 0, here + by < size))
            def _():
                pl.semaphore_signal(
                    barrier, inc=1, device_id={axis: here + by},
                    device_id_type=pl.DeviceIdType.MESH,
                )

    pairs = [
        (psf_hbm.at[:, :, 0, :], psf_ref), (data_hbm, data_ref), (precond_hbm, precond_ref),
        (kernel_hbm, kernel_ref), (field_hbm, field_ref), (back_hbm, back_ref),
    ]
    loads = [pltpu.make_async_copy(a, b, load_sem.at[k]) for k, (a, b) in enumerate(pairs)]
    for load in loads:
        load.start()

    wide[...] = jnp.zeros(wide.shape, wide.dtype)
    packed[...] = jnp.zeros(packed.shape, packed.dtype)
    every = slice(None)
    edges = [
        (gx == 0, (pl.ds(0, half), every)), (gx == size_x - 1, (pl.ds(half + count_x, half), every)),
        (gy == 0, (every, pl.ds(0, half))), (gy == size_y - 1, (every, pl.ds(half + count_y, half))),
    ]
    for edge, at in edges:
        @pl.when(edge)
        def _():
            for region in regions:
                region[at] = jnp.zeros(region[at].shape, region.dtype)

    loads[0].wait()
    for a in range(width):
        wide[a, pl.ds(0, width), pl.ds(0, width)] = psf_ref[a]
    for n in range(nodes.shape[1]):
        total = wide[n * per]
        for a in range(n * per + 1, min(width, (n + 1) * per)):
            total = total + pltpu.roll(wide[a], width * (a % per), axis=1)
        nodes[0, n] = total
    loads[1].wait()
    loads[2].wait()
    own = (pl.ds(half, count_x), pl.ds(half, count_y))
    region0[own] = precond_ref[...] * data_ref[...]

    peers = 0
    for here, size in ((gx, size_x), (gy, size_y)):
        peers += (here > 0).astype(jnp.int32) + (here < size - 1).astype(jnp.int32)
    pl.semaphore_wait(barrier, peers)

    inline = Link(sems, 0, nodes.at[0], nodes.at[1], "gx", -1)
    cross = Link(sems, 1, nodes.at[0], nodes.at[2], "gy", -1)
    corner = Link(sems, 2, nodes.at[2], nodes.at[3], "gx", -1, gy < size_y - 1)
    cross.start()
    inline.start()
    started = [cross, inline, corner]
    last_x, last_y = gx == size_x - 1, gy == size_y - 1
    links = [
        halo_links(regions[n], count_x, count_y, half, sems, 3 + LINKS * n) for n in range(ITERS)
    ]
    for along_y, along_x, relayed in links:
        started += sum(along_y + along_x + relayed, [])

    def send(along_y, along_x):
        for link in along_y + along_x:
            link.start()

    def pack(count, place, node):
        packed[:, pl.ds(place * full, full), :] = nodes[node, :, pl.ds(0, full), :]
        packed[:, pl.ds(count * full + place, 1), :] = nodes[node, :, pl.ds(full, 1), :]

    def node_spectra(count, first, k2):
        spectra(
            count, width, region_x, region_y, first, packed, kernel_ref, g_ref, k1, k2, left, work
        )

    def inline_tiles(count, tile_of):
        @pl.loop(0, count)
        def _(n):
            inline_forward(tile_of(n), region_x, region_y, pitch, z, c, work)

    def own_forward(region, along_x):
        depth_forward(region, (half, count_x, half, count_y), field_ref, z)
        for link in along_x[0] + along_x[1]:
            link.wait_recv()
        depth_forward(region, (0, half, half, count_y), field_ref, z)
        depth_forward(region, (half + count_x, half, half, count_y), field_ref, z)
        inline_tiles(count_y // SUB, lambda n: n + half // SUB)

    def relay(along_y, relayed, k):
        for n in range(2):
            along_y[n][k].wait_recv()
            for parity in range(2):
                pl.when((gx + k) % 2 == parity)(relayed[n][parity].start)

    def halo_forward(region, relayed):
        depth_forward(region, (half, count_x, 0, half), field_ref, z)
        depth_forward(region, (half, count_x, half + count_y, half), field_ref, z)
        for link in relayed[0] + relayed[1]:
            link.wait_recv()
        for x0 in (0, half + count_x):
            for y0 in (0, half + count_y):
                depth_forward(region, (x0, half, y0, half), field_ref, z)
        edge, skip = half // SUB, count_y // SUB
        inline_tiles(2 * edge, lambda n: n + (n // edge) * skip)

    def operator(present):
        crossline(present, count_y, region_x, region_y, pitch, g_ref, c, v, u, work)

    def finish(sweep_index):
        region, last = regions[sweep_index], sweep_index == ITERS - 1
        tiles = count_y // SUB
        for tile in range(tiles):
            inline_back(tile, count_x, region_x, pitch, u, w, work)
            blended = product(w[tile], back_ref[...])
            here = pl.ds(tile * SUB, SUB)
            inner = pl.ds(half + tile * SUB, SUB)
            for x in range(count_x):
                model = region[x + half, inner, :]
                residual = data_ref[x, here, :] - (model + blended[x * SUB : (x + 1) * SUB])
                model = model + relaxation * precond_ref[x, here, :] * residual
                if last:
                    residual_ref[x, here, :] = residual
                    model_ref[x, here, :] = model
                else:
                    regions[sweep_index + 1][x + half, inner, :] = model
            if not last and (tile + 1) % (tiles // 2) == 0:
                n = (tile + 1) // (tiles // 2) - 1
                along_y, along_x, _ = links[sweep_index + 1]
                send(along_y[n], along_x[n])

    along_y, along_x, relayed = links[0]
    send([], along_x[0] + along_x[1])
    send([along_y[0][0], along_y[1][0], along_y[0][1], along_y[1][1]], [])
    loads[3].wait()
    pack(2, 0, 0)
    inline.wait_recv()
    pl.when(last_x)(lambda: pack(2, 1, 0))
    pl.when(jnp.logical_not(last_x))(lambda: pack(2, 1, 1))
    node_spectra(2, 0, k2a)
    loads[4].wait()
    loads[5].wait()
    own_forward(region0, along_x)
    cross.wait_recv()
    corner.start()
    pl.when(last_y)(lambda: pack(1, 0, 0))
    pl.when(jnp.logical_not(last_y))(lambda: pack(1, 0, 2))
    node_spectra(1, 2, k2b)
    corner.wait_recv()
    for edge_x in (False, True):
        for edge_y in (False, True):
            here = (last_x if edge_x else jnp.logical_not(last_x),
                    last_y if edge_y else jnp.logical_not(last_y))
            source = (0 if edge_y else 2) if edge_x else (1 if edge_y else 3)
            pl.when(jnp.logical_and(*here))(lambda: pack(1, 0, source))
    relay(along_y, relayed, 0)
    node_spectra(1, 3, k2c)
    relay(along_y, relayed, 1)
    halo_forward(region0, relayed)
    operator(range(region_y))
    finish(0)
    for sweep_index in range(1, ITERS):
        region = regions[sweep_index]
        along_y, along_x, relayed = links[sweep_index]
        own_forward(region, along_x)
        operator(range(half, half + count_y))
        if sweep_index == 1:
            places = [(k2a, 2, 0), (k2a, 2, 1), (k2b, 1, 0), (k2c, 1, 0)]
            blend_kernels(half, count_x, count_y, places, kb)
        relay(along_y, relayed, 0)
        relay(along_y, relayed, 1)
        halo_forward(region, relayed)
        add_halo(half, count_x, count_y, pitch, c, kb, u)
        finish(sweep_index)
    for link in started:
        link.wait_send()


def local(data, precond, psf):
    count_x, count_y, depth = data.shape
    width = psf.shape[2]
    half = width // 2
    region_x, region_y = count_x + 2 * half, count_y + 2 * half
    field, kernel, back = tables(depth, width)
    back = back / (region_x * region_y)
    f32 = jnp.float32
    up = lambda n, m: -(-n // m) * m
    high, columns = up(width, SUB), up(width, LANES // width) // (LANES // width)
    rows, single = rows_of(2, width), rows_of(1, width)
    terms = len(halo_terms(half, count_y))
    pitch = max(region_x, region_y) + SUB
    vmem = lambda *shape: pltpu.VMEM(shape, f32)
    table = lambda *shape: pltpu.VMEM(shape, jnp.bfloat16)
    square = region_x * region_y
    flat = psf.transpose(0, 2, 3, 1, 4).reshape(width, width, 1, width)
    operands = (data, precond, flat, stacked(field), stacked(kernel), stacked(back))
    model, residual = pl.pallas_call(
        functools.partial(whole_kernel, count_x, count_y, half, pitch),
        out_shape=[jax.ShapeDtypeStruct(data.shape, f32)] * 2,
        in_specs=[pl.BlockSpec(memory_space=pltpu.HBM)] * 6,
        out_specs=[pl.BlockSpec(memory_space=pltpu.VMEM)] * 2,
        scratch_shapes=[
            vmem(*data.shape),
            vmem(*data.shape),
            vmem(width, width, width),
            table(*operands[3].shape),
            table(*operands[4].shape),
            table(*operands[5].shape),
            vmem(region_x, region_y, depth),
            vmem(region_x, region_y, depth),
            vmem(width, high, LANES),
            vmem(4, columns, high, LANES),
            vmem(columns, rows, LANES),
            vmem(width * rows, LANES),
            vmem(4, 2, square, LANES),
            vmem(2, width * rows, LANES),
            vmem(2, region_x * rows, LANES),
            vmem(2, region_x * single, LANES),
            vmem(2, region_x * single, LANES),
            vmem(2, region_x // SUB, terms, 2, SUB, LANES),
            vmem(2, square, LANES),
            vmem(2, region_x * pitch, LANES),
            vmem(2, region_y, SUB, LANES),
            vmem(2, 2, count_y * pitch, LANES),
            vmem(count_y // SUB, count_x * SUB, 2 * LANES),
            vmem(2, 2, max(region_x, region_y), SUB, LANES),
            pltpu.SemaphoreType.DMA((6,)),
            pltpu.SemaphoreType.DMA((3 + LINKS * ITERS,)),
            pltpu.SemaphoreType.DMA((3 + LINKS * ITERS,)),
        ],
        compiler_params=pltpu.CompilerParams(
            vmem_limit_bytes=54976 << 10, collective_id=0, has_side_effects=True
        ),
        name="whole",
    )(*operands)
    def tail(a, b, c, e, sems):
        copies = [pltpu.make_async_copy(a, c, sems.at[0]), pltpu.make_async_copy(b, e, sems.at[1])]
        for copy in copies:
            copy.start()
        for copy in copies:
            copy.wait()

    return pl.pallas_call(
        tail,
        out_shape=[jax.ShapeDtypeStruct(data.shape, f32)] * 2,
        in_specs=[pl.BlockSpec(memory_space=pltpu.VMEM)] * 2,
        out_specs=[pl.BlockSpec(memory_space=pl.ANY)] * 2,
        scratch_shapes=[pltpu.SemaphoreType.DMA((2,))],
        compiler_params=pltpu.CompilerParams(vmem_limit_bytes=54976 << 10),
        name="tail",
    )(model, residual)


def solution(mesh):
    placed = (P("gx", "gy", None), P("gx", "gy", None), P("gx", "gy", None, None, None))
    return jax.shard_map(
        local,
        mesh=mesh,
        in_specs=placed,
        out_specs=(P("gx", "gy", None), P("gx", "gy", None)),
        check_vma=False,
    )
```

```python
import functools
import math

import jax
import jax.numpy as jnp
import numpy as np
from jax import lax
from jax.experimental import pallas as pl
from jax.experimental.pallas import tpu as pltpu
from jax.sharding import PartitionSpec as P

ITERS = 2
relaxation = 0.7
LANES = 128
SUB = 8
OUTER = 4


def times_phase(value, turn, size, sign):
    if value is None:
        return None
    re, im = value
    turn = (sign * turn) % size
    eighth = 8 * turn
    if eighth == 0:
        return value
    if eighth == 2 * size:
        return (-im, re)
    if eighth == 4 * size:
        return (-re, -im)
    if eighth == 6 * size:
        return (im, -re)
    angle = 2.0 * math.pi * turn / size
    cosine, sine = math.cos(angle), math.sin(angle)
    if eighth % size == 0:
        root = math.sqrt(0.5)
        first, second = (re - im) * root, (re + im) * root
        if eighth == size:
            return (first, second)
        if eighth == 3 * size:
            return (-second, first)
        if eighth == 5 * size:
            return (-first, -second)
        return (second, -first)
    return (re * cosine - im * sine, re * sine + im * cosine)


def plus(a, b):
    if a is None:
        return b
    if b is None:
        return a
    return (a[0] + b[0], a[1] + b[1])


def minus(a, b):
    if b is None:
        return a
    if a is None:
        return (-b[0], -b[1])
    return (a[0] - b[0], a[1] - b[1])


def transform(values, sign, wanted):
    size = len(values)
    if all(v is None for v in values):
        return [None] * wanted
    if size == 1:
        return list(values)
    half = size // 2
    if size % 2:
        raise ValueError("length")
    even = transform(values[0::2], sign, min(half, wanted))
    odd = transform(values[1::2], sign, min(half, wanted))
    odd = [times_phase(v, k, size, sign) for k, v in enumerate(odd)]
    low = [plus(a, b) for a, b in zip(even, odd)]
    high = [minus(a, b) for a, b in zip(even, odd)]
    return (low + high)[:wanted]


def tables(depth, width):
    half = width // 2
    length = depth + 2 * half
    count = length // 2 + 1
    k = np.arange(count)
    field = np.zeros((depth, 2 * LANES))
    turns = (np.arange(depth)[:, None] + half) * k[None, :] % length
    angle = turns * (2.0 * np.pi / length)
    field[:, :count] = np.cos(angle)
    field[:, LANES : LANES + count] = -np.sin(angle)
    kernel = np.zeros((LANES, 2 * LANES))
    angle = np.arange(width)[:, None] * k[None, :] % length * (2.0 * np.pi / length)
    kernel[:width, :count] = np.cos(angle)
    kernel[:width, LANES : LANES + count] = np.sin(angle)
    back = np.zeros((2 * LANES, depth))
    weight = np.where((k == 0) | (2 * k == length), 1.0, 2.0) / length
    angle = k[:, None] * np.arange(depth)[None, :] % length * (2.0 * np.pi / length)
    back[:count] = weight[:, None] * np.cos(angle)
    back[LANES : LANES + count] = -weight[:, None] * np.sin(angle)
    return field, kernel, back


def stacked(table):
    high = jnp.asarray(table, jnp.float32).astype(jnp.bfloat16)
    low = (jnp.asarray(table, jnp.float32) - high.astype(jnp.float32)).astype(jnp.bfloat16)
    return jnp.concatenate([high, high, low])


def product(left, table):
    high = left.astype(jnp.bfloat16)
    low = (left - high.astype(jnp.float32)).astype(jnp.bfloat16)
    left = jnp.concatenate([high, low, high], axis=1)
    rows = left.shape[0]
    cut = rows // 2 // (2 * SUB) * (2 * SUB)
    dot = lambda part: jnp.dot(part, table, preferred_element_type=jnp.float32)
    return jnp.concatenate([dot(left[:cut]), dot(left[cut:])]) if cut else dot(left)


def first_pass(load, keep, size, sign):
    inner = size // OUTER
    for r in range(OUTER):
        values = transform([load(OUTER * a + r) for a in range(inner)], sign, inner)
        for m, value in enumerate(values):
            keep(r * inner + m, times_phase(value, r * m, size, sign))


def second_pass(kept, size, sign, wanted):
    inner = size // OUTER
    for m in range(inner):
        values = [kept(r * inner + m) for r in range(OUTER)]
        for q, value in enumerate(transform(values, sign, wanted // inner)):
            yield m + inner * q, value


def keeper(buffer, slot):
    def keep(n, value):
        buffer[slot, 0, n], buffer[slot, 1, n] = value

    def kept(n):
        return buffer[slot, 0, n], buffer[slot, 1, n]

    return keep, kept


def rows_of(count, width):
    return -(-count * width // SUB) * SUB


def row_of(count, width, node, b):
    full = width - 1
    return node * full + b if b < full else count * full + node


def spectra(count, width, region_x, region_y, first, packed, table_ref, g_ref, k1, k2, left, work, between):
    per, rows = LANES // width, rows_of(count, width)
    for a in range(width):
        shifted = packed[a // per, pl.ds(0, rows), :]
        if a % per:
            shifted = pltpu.roll(shifted, LANES - width * (a % per), axis=1)
        left[pl.ds(a * rows, rows), :] = shifted
    both = product(left[pl.ds(0, width * rows), :], table_ref[...])
    k1[0, pl.ds(0, width * rows), :] = both[:, :LANES]
    k1[1, pl.ds(0, width * rows), :] = both[:, LANES:]

    @pl.loop(0, rows // SUB)
    def _(tile):
        at = lambda i: pl.ds(pl.multiple_of(i * rows + tile * SUB, SUB), SUB)
        load = lambda a: (k1[0, at(a), :], k1[1, at(a), :]) if a < width else None
        keep, kept = keeper(work, 0)
        first_pass(load, keep, region_x, 1)
        for kx, (re, im) in second_pass(kept, region_x, 1, region_x):
            k2[0, at(kx), :] = re
            k2[1, at(kx), :] = im

    between()
    for node in range(count):
        @pl.loop(0, region_x // SUB)
        def _(tile):
            def load(b):
                if b >= width:
                    return None
                row = row_of(count, width, node, b)
                at = pl.ds(tile * SUB * rows + row, SUB, stride=rows)
                return k2[0, at, :], k2[1, at, :]

            keep, kept = keeper(work, 0)
            first_pass(load, keep, region_y, 1)
            for ky, (re, im) in second_pass(kept, region_y, 1, region_y):
                to = pl.ds(pl.multiple_of(ky * region_x + tile * SUB, SUB), SUB)
                g_ref[first + node, 0, to, :] = re
                g_ref[first + node, 1, to, :] = im


def halo_terms(half, count_y):
    terms = []
    for y in range(half):
        terms += [(y, y + b, b) for b in range(half - y)]
    for y in range(count_y - half, count_y):
        first = half + count_y
        terms += [(y, n, n - y) for n in range(first, y + 2 * half + 1)]
    return terms


def blend_kernels(half, count_x, count_y, places, kb):
    region_x, region_y = count_x + 2 * half, count_y + 2 * half
    width = 2 * half + 1
    terms = halo_terms(half, count_y)

    @pl.loop(0, region_x // SUB)
    def _(tile):
        for i in range(2):
            def kernel(j, b):
                ref, count, node = places[2 * j + i]
                rows = rows_of(count, width)
                at = pl.ds(tile * SUB * rows + row_of(count, width, node, b), SUB, stride=rows)
                return ref[0, at, :], ref[1, at, :]

            for b in range(width):
                mine = [(n, y) for n, (y, _, lag) in enumerate(terms) if lag == b]
                if not mine:
                    continue
                (ar, ai), (br, bi) = kernel(0, b), kernel(1, b)
                for n, y in mine:
                    t = (y + 0.5) / count_y
                    low, high = region_y * (1.0 - t), region_y * t
                    kb[i, tile, n, 0] = low * ar + high * br
                    kb[i, tile, n, 1] = low * ai + high * bi


def add_halo(half, count_x, count_y, pitch, c, kb, u):
    region_x, region_y = count_x + 2 * half, count_y + 2 * half
    terms = list(enumerate(halo_terms(half, count_y)))

    @pl.loop(0, region_x // SUB)
    def _(tile):
        for side in (range(half), range(half + count_y, region_y)):
            halo = {}
            for n in side:
                at = pl.ds(tile * SUB * pitch + n, SUB, stride=pitch)
                halo[n] = c[0, at, :], c[1, at, :]
            for i in range(2):
                for y in range(count_y):
                    mine = [(k, n) for k, (to, n, _) in terms if to == y and n in halo]
                    if not mine:
                        continue
                    at = pl.ds(pl.multiple_of(y * pitch + tile * SUB, SUB), SUB)
                    re, im = u[i, 0, at, :], u[i, 1, at, :]
                    for k, n in mine:
                        kr, ki = kb[i, tile, k, 0], kb[i, tile, k, 1]
                        vr, vi = halo[n]
                        re = re + (vr * kr - vi * ki)
                        im = im + (vr * ki + vi * kr)
                    u[i, 0, at, :] = re
                    u[i, 1, at, :] = im


def depth_forward(region, box, field_ref, z):
    x0, nx, y0, ny = box
    region_y = region.shape[1]
    step = max(1, 2 * LANES // ny)
    for x in range(x0, x0 + nx, step):
        count = min(step, x0 + nx - x)
        left = region[pl.ds(x, count), pl.ds(y0, ny), :].reshape(count * ny, LANES)
        both = product(left, field_ref[...])
        for i in range(count):
            to = pl.ds((x + i) * region_y + y0, ny)
            z[0, to, :] = both[i * ny : (i + 1) * ny, :LANES]
            z[1, to, :] = both[i * ny : (i + 1) * ny, LANES:]


def inline_forward(tile, region_x, region_y, pitch, z, c, work):
    def load(x):
        at = pl.ds(pl.multiple_of(x * region_y + tile * SUB, SUB), SUB)
        return z[0, at, :], z[1, at, :]

    keep, kept = keeper(work, 0)
    first_pass(load, keep, region_x, -1)
    for kx, (re, im) in second_pass(kept, region_x, -1, region_x):
        to = pl.ds(pl.multiple_of(kx * pitch + tile * SUB, SUB), SUB)
        c[0, to, :] = re
        c[1, to, :] = im


def crossline(present, nodes, count_y, region_x, region_y, pitch, g_ref, c, v, u, work):
    more = nodes[0] > 0

    @pl.loop(0, region_x // SUB)
    def _(tile):
        def load(y):
            if y not in present:
                return None
            at = pl.ds(tile * SUB * pitch + y, SUB, stride=pitch)
            return c[0, at, :], c[1, at, :]

        if not more:
            keep, kept = keeper(work, 0)
            first_pass(load, keep, region_y, -1)
            for ky, (re, im) in second_pass(kept, region_y, -1, region_y):
                v[tile, 0, ky] = re
                v[tile, 1, ky] = im

        @pl.loop(0, 2)
        def _(i):
            for j in nodes:
                def load(ky):
                    at = pl.ds(pl.multiple_of(ky * region_x + tile * SUB, SUB), SUB)
                    gr, gi = g_ref[2 * j + i, 0, at, :], g_ref[2 * j + i, 1, at, :]
                    vr, vi = v[tile, 0, ky], v[tile, 1, ky]
                    return vr * gr - vi * gi, vr * gi + vi * gr

                keep, _ = keeper(work, j)
                first_pass(load, keep, region_y, 1)
            passes = [second_pass(keeper(work, j)[1], region_y, 1, count_y) for j in nodes]
            for found in zip(*passes):
                y = found[0][0]
                to = pl.ds(pl.multiple_of(y * pitch + tile * SUB, SUB), SUB)
                parts = [(u[i, 0, to, :], u[i, 1, to, :])] if more else []
                for j, (_, (re, im)) in zip(nodes, found):
                    t = (y + 0.5) / count_y
                    weight = t if j else 1.0 - t
                    parts.append((weight * re, weight * im))
                re, im = functools.reduce(plus, parts)
                u[i, 0, to, :] = re
                u[i, 1, to, :] = im


def inline_back(tile, count_x, region_x, pitch, u, w, work):
    for i in range(2):
        def load(kx):
            at = pl.ds(tile * SUB * pitch + kx, SUB, stride=pitch)
            return u[i, 0, at, :], u[i, 1, at, :]

        keep, _ = keeper(work, i)
        first_pass(load, keep, region_x, 1)
    passes = [second_pass(keeper(work, i)[1], region_x, 1, count_x) for i in range(2)]
    for (x, (ar, ai)), (_, (br, bi)) in zip(*passes):
        s = (x + 0.5) / count_x
        w[tile, pl.ds(x * SUB, SUB), :LANES] = (1.0 - s) * ar + s * br
        w[tile, pl.ds(x * SUB, SUB), LANES:] = (1.0 - s) * ai + s * bi


class Link:
    def __init__(self, sems, k, src, dst, only=True, **by):
        self.sends, self.gets, there = only, only, {}
        for axis, step in by.items():
            here, size = lax.axis_index(axis), lax.axis_size(axis)
            inside = lambda i: jnp.logical_and(i >= 0, i < size)
            self.sends = jnp.logical_and(self.sends, inside(here + step))
            self.gets = jnp.logical_and(self.gets, inside(here - step))
            there[axis] = here + step
        self.copy = pltpu.make_async_remote_copy(
            src_ref=src, dst_ref=dst, send_sem=sems[0].at[k], recv_sem=sems[1].at[k],
            device_id=there, device_id_type=pl.DeviceIdType.MESH,
        )

    def start(self):
        pl.when(self.sends)(lambda: self.copy.start())

    def wait_recv(self):
        pl.when(self.gets)(lambda: self.copy.wait_recv())

    def wait_send(self):
        pl.when(self.sends)(lambda: self.copy.wait_send())


LINKS = 12


def halo_links(region, count_x, count_y, half, sems, base, direct):
    gx, gy, size = lax.axis_index("gx"), lax.axis_index("gy"), lax.axis_size("gy")
    low, high_x, high_y = pl.ds(0, half), pl.ds(half + count_x, half), pl.ds(half + count_y, half)
    last_x, last_y, first = pl.ds(count_x, half), pl.ds(count_y, half), pl.ds(half, half)
    at = lambda x, y: region.at[x, y]
    part_x, part_y = count_x // 2, count_y // 2
    along_y = []
    for n, (src, dst, by) in enumerate(((first, high_y, -1), (last_y, low, 1))):
        along_y.append([])
        for k in range(2):
            x = pl.ds(half + part_x * ((gx + 1 + k) % 2), part_x)
            along_y[n].append(Link(sems, base + 2 * n + k, at(x, src), at(x, dst), gy=by))
    along_x = []
    for n in range(2):
        part = pl.ds(half + n * part_y, part_y)
        along_x.append([
            Link(sems, base + 4 + 2 * n, at(last_x, part), at(low, part), gx=1),
            Link(sems, base + 5 + 2 * n, at(first, part), at(high_x, part), gx=-1),
        ])
    relayed = []
    sides = ((high_y, first, -1, gy < size - 1), (low, last_y, 1, gy > 0))
    for n, (dst, src, by, has) in enumerate(sides):
        if direct:
            up = Link(sems, base + 8 + 2 * n, at(low, src), at(low, dst), gx > 0, gy=by)
        else:
            up = Link(sems, base + 8 + 2 * n, at(last_x, dst), at(low, dst), has, gx=1)
        down = Link(sems, base + 9 + 2 * n, at(first, dst), at(high_x, dst), has, gx=-1)
        relayed.append([up, down])
    return along_y, along_x, relayed


def whole_kernel(
    count_x, count_y, half, pitch,
    data_hbm, precond_hbm, psf_hbm, field_hbm, kernel_hbm, back_hbm,
    model_ref, residual_ref,
    data_ref, precond_ref, psf_ref, field_ref, kernel_ref, back_ref,
    region0, region1, wide, nodes, packed, left, g_ref, k1, k2a, k2b, k2c, kb, z, c, v, u, w, work,
    load_sem, send_sem, recv_sem,
):
    width = 2 * half + 1
    full = width - 1
    per = LANES // width
    region_x, region_y = count_x + 2 * half, count_y + 2 * half
    sems = (send_sem, recv_sem)
    gx, gy = lax.axis_index("gx"), lax.axis_index("gy")
    size_x, size_y = lax.axis_size("gx"), lax.axis_size("gy")
    regions = [region0, region1]

    barrier = pltpu.get_barrier_semaphore()
    for axis, here, size in (("gx", gx, size_x), ("gy", gy, size_y)):
        for by in (-1, 1):
            @pl.when(jnp.logical_and(here + by >= 0, here + by < size))
            def _():
                pl.semaphore_signal(
                    barrier, inc=1, device_id={axis: here + by},
                    device_id_type=pl.DeviceIdType.MESH,
                )

    pairs = [
        (psf_hbm.at[:, :, 0, :], psf_ref), (data_hbm, data_ref), (precond_hbm, precond_ref),
        (kernel_hbm, kernel_ref), (field_hbm, field_ref), (back_hbm, back_ref),
    ]
    loads = [pltpu.make_async_copy(a, b, load_sem.at[k]) for k, (a, b) in enumerate(pairs)]
    for load in loads:
        load.start()

    wide[...] = jnp.zeros(wide.shape, wide.dtype)
    packed[...] = jnp.zeros(packed.shape, packed.dtype)
    every = slice(None)
    edges = [
        (gx == 0, (pl.ds(0, half), every)), (gx == size_x - 1, (pl.ds(half + count_x, half), every)),
        (gy == 0, (every, pl.ds(0, half))), (gy == size_y - 1, (every, pl.ds(half + count_y, half))),
    ]
    for edge, at in edges:
        @pl.when(edge)
        def _():
            for region in regions:
                region[at] = jnp.zeros(region[at].shape, region.dtype)

    loads[0].wait()
    for a in range(width):
        wide[a, pl.ds(0, width), pl.ds(0, width)] = psf_ref[a]
    for n in range(nodes.shape[1]):
        total = wide[n * per]
        for a in range(n * per + 1, min(width, (n + 1) * per)):
            total = total + pltpu.roll(wide[a], width * (a % per), axis=1)
        nodes[0, n] = total
    loads[1].wait()
    loads[2].wait()
    own = (pl.ds(half, count_x), pl.ds(half, count_y))
    region0[own] = precond_ref[...] * data_ref[...]

    peers = 0
    for here, size in ((gx, size_x), (gy, size_y)):
        peers += (here > 0).astype(jnp.int32) + (here < size - 1).astype(jnp.int32)
    pl.semaphore_wait(barrier, peers)

    inline = Link(sems, 0, nodes.at[0], nodes.at[1], gx=-1)
    cross = Link(sems, 1, nodes.at[0], nodes.at[2], gy=-1)
    corner = Link(sems, 2, nodes.at[2], nodes.at[3], gy < size_y - 1, gx=-1)
    cross.start()
    inline.start()
    started = [cross, inline, corner]
    last_x, last_y = gx == size_x - 1, gy == size_y - 1
    links = [
        halo_links(regions[n], count_x, count_y, half, sems, 3 + LINKS * n, n > 0)
        for n in range(ITERS)
    ]
    for along_y, along_x, relayed in links:
        started += sum(along_y + along_x + relayed, [])

    def send(links):
        for link in links:
            link.start()

    def pack(count, place, node):
        packed[:, pl.ds(place * full, full), :] = nodes[node, :, pl.ds(0, full), :]
        packed[:, pl.ds(count * full + place, 1), :] = nodes[node, :, pl.ds(full, 1), :]

    def node_spectra(count, first, k2, between=lambda: None):
        spectra(
            count, width, region_x, region_y, first, packed, kernel_ref, g_ref, k1, k2, left, work,
            between,
        )

    def inline_tiles(count, tile_of):
        @pl.loop(0, count)
        def _(n):
            inline_forward(tile_of(n), region_x, region_y, pitch, z, c, work)

    def own_forward(region, along_x, after=()):
        depth_forward(region, (half, count_x, half, count_y), field_ref, z)
        for link in along_x[0] + along_x[1]:
            link.wait_recv()
        send(after)
        depth_forward(region, (0, half, half, count_y), field_ref, z)
        depth_forward(region, (half + count_x, half, half, count_y), field_ref, z)
        inline_tiles(count_y // SUB, lambda n: n + half // SUB)

    def relay(along_y, relayed, k, direct=False):
        for n in range(2):
            along_y[n][k].wait_recv()
            for parity in range(int(direct), 2):
                pl.when((gx + k) % 2 == parity)(relayed[n][parity].start)

    def halo_forward(region, relayed):
        depth_forward(region, (half, count_x, 0, half), field_ref, z)
        depth_forward(region, (half, count_x, half + count_y, half), field_ref, z)
        for link in relayed[0] + relayed[1]:
            link.wait_recv()
        for x0 in (0, half + count_x):
            for y0 in (0, half + count_y):
                depth_forward(region, (x0, half, y0, half), field_ref, z)
        edge, skip = half // SUB, count_y // SUB
        inline_tiles(2 * edge, lambda n: n + (n // edge) * skip)

    def operator(*nodes):
        own = range(half, half + count_y)
        crossline(own, nodes, count_y, region_x, region_y, pitch, g_ref, c, v, u, work)

    def finish(sweep_index):
        region, last = regions[sweep_index], sweep_index == ITERS - 1
        tiles = count_y // SUB
        for tile in range(tiles):
            inline_back(tile, count_x, region_x, pitch, u, w, work)
            blended = product(w[tile], back_ref[...])
            here = pl.ds(tile * SUB, SUB)
            inner = pl.ds(half + tile * SUB, SUB)
            for x in range(count_x):
                model = region[x + half, inner, :]
                residual = data_ref[x, here, :] - (model + blended[x * SUB : (x + 1) * SUB])
                model = model + relaxation * precond_ref[x, here, :] * residual
                if last:
                    residual_ref[x, here, :] = residual
                    model_ref[x, here, :] = model
                else:
                    regions[sweep_index + 1][x + half, inner, :] = model
            if not last and (tile + 1) % (tiles // 2) == 0:
                n = (tile + 1) // (tiles // 2) - 1
                along_y, along_x, _ = links[sweep_index + 1]
                send(along_x[n] + [along_y[n][0]])
                if n:
                    send([along_y[0][1], along_y[1][1]])

    along_y, along_x, relayed = links[0]
    send(along_x[0] + along_x[1])
    send([along_y[0][0], along_y[1][0], along_y[0][1], along_y[1][1]])
    loads[3].wait()
    pack(2, 0, 0)
    inline.wait_recv()
    pl.when(last_x)(lambda: pack(2, 1, 0))
    pl.when(jnp.logical_not(last_x))(lambda: pack(2, 1, 1))
    node_spectra(2, 0, k2a)
    loads[4].wait()
    loads[5].wait()
    own_forward(region0, along_x)
    operator(0)
    cross.wait_recv()
    corner.start()
    pl.when(last_y)(lambda: pack(1, 0, 0))
    pl.when(jnp.logical_not(last_y))(lambda: pack(1, 0, 2))
    node_spectra(1, 2, k2b)
    corner.wait_recv()
    for edge_x in (False, True):
        for edge_y in (False, True):
            here = (last_x if edge_x else jnp.logical_not(last_x),
                    last_y if edge_y else jnp.logical_not(last_y))
            source = (0 if edge_y else 2) if edge_x else (1 if edge_y else 3)
            pl.when(jnp.logical_and(*here))(lambda: pack(1, 0, source))
    node_spectra(1, 3, k2c, lambda: relay(along_y, relayed, 0))
    operator(1)
    relay(along_y, relayed, 1)
    places = [(k2a, 2, 0), (k2a, 2, 1), (k2b, 1, 0), (k2c, 1, 0)]
    blend_kernels(half, count_x, count_y, places, kb)
    halo_forward(region0, relayed)
    add_halo(half, count_x, count_y, pitch, c, kb, u)
    finish(0)
    for sweep_index in range(1, ITERS):
        region = regions[sweep_index]
        along_y, along_x, relayed = links[sweep_index]
        own_forward(region, along_x, [relayed[0][0], relayed[1][0]])
        operator(0, 1)
        relay(along_y, relayed, 0, True)
        relay(along_y, relayed, 1, True)
        halo_forward(region, relayed)
        add_halo(half, count_x, count_y, pitch, c, kb, u)
        finish(sweep_index)
    for link in started:
        link.wait_send()


def local(data, precond, psf):
    count_x, count_y, depth = data.shape
    width = psf.shape[2]
    half = width // 2
    region_x, region_y = count_x + 2 * half, count_y + 2 * half
    field, kernel, back = tables(depth, width)
    back = back / (region_x * region_y)
    f32 = jnp.float32
    up = lambda n, m: -(-n // m) * m
    high, columns = up(width, SUB), up(width, LANES // width) // (LANES // width)
    rows, single = rows_of(2, width), rows_of(1, width)
    terms = len(halo_terms(half, count_y))
    pitch = max(region_x, region_y) + SUB
    vmem = lambda *shape: pltpu.VMEM(shape, f32)
    table = lambda *shape: pltpu.VMEM(shape, jnp.bfloat16)
    square = region_x * region_y
    flat = psf.transpose(0, 2, 3, 1, 4).reshape(width, width, 1, width)
    operands = (data, precond, flat, stacked(field), stacked(kernel), stacked(back))
    model, residual = pl.pallas_call(
        functools.partial(whole_kernel, count_x, count_y, half, pitch),
        out_shape=[jax.ShapeDtypeStruct(data.shape, f32)] * 2,
        in_specs=[pl.BlockSpec(memory_space=pltpu.HBM)] * 6,
        out_specs=[pl.BlockSpec(memory_space=pltpu.VMEM)] * 2,
        scratch_shapes=[
            vmem(*data.shape),
            vmem(*data.shape),
            vmem(width, width, width),
            table(*operands[3].shape),
            table(*operands[4].shape),
            table(*operands[5].shape),
            vmem(region_x, region_y, depth),
            vmem(region_x, region_y, depth),
            vmem(width, high, LANES),
            vmem(4, columns, high, LANES),
            vmem(columns, rows, LANES),
            vmem(width * rows, LANES),
            vmem(4, 2, square, LANES),
            vmem(2, width * rows, LANES),
            vmem(2, region_x * rows, LANES),
            vmem(2, region_x * single, LANES),
            vmem(2, region_x * single, LANES),
            vmem(2, region_x // SUB, terms, 2, SUB, LANES),
            vmem(2, square, LANES),
            vmem(2, region_x * pitch, LANES),
            vmem(region_x // SUB, 2, region_y, SUB, LANES),
            vmem(2, 2, count_y * pitch, LANES),
            vmem(count_y // SUB, count_x * SUB, 2 * LANES),
            vmem(2, 2, max(region_x, region_y), SUB, LANES),
            pltpu.SemaphoreType.DMA((6,)),
            pltpu.SemaphoreType.DMA((3 + LINKS * ITERS,)),
            pltpu.SemaphoreType.DMA((3 + LINKS * ITERS,)),
        ],
        compiler_params=pltpu.CompilerParams(
            vmem_limit_bytes=54976 << 10, collective_id=0, has_side_effects=True
        ),
        name="whole",
    )(*operands)
    def tail(a, b, c, e, sems):
        copies = [pltpu.make_async_copy(a, c, sems.at[0]), pltpu.make_async_copy(b, e, sems.at[1])]
        for copy in copies:
            copy.start()
        for copy in copies:
            copy.wait()

    return pl.pallas_call(
        tail,
        out_shape=[jax.ShapeDtypeStruct(data.shape, f32)] * 2,
        in_specs=[pl.BlockSpec(memory_space=pltpu.VMEM)] * 2,
        out_specs=[pl.BlockSpec(memory_space=pl.ANY)] * 2,
        scratch_shapes=[pltpu.SemaphoreType.DMA((2,))],
        compiler_params=pltpu.CompilerParams(vmem_limit_bytes=54976 << 10),
        name="tail",
    )(model, residual)


def solution(mesh):
    placed = (P("gx", "gy", None), P("gx", "gy", None), P("gx", "gy", None, None, None))
    return jax.shard_map(
        local,
        mesh=mesh,
        in_specs=placed,
        out_specs=(P("gx", "gy", None), P("gx", "gy", None)),
        check_vma=False,
    )
```

```python
import functools
import math

import jax
import jax.numpy as jnp
import numpy as np
from jax import lax
from jax.experimental import pallas as pl
from jax.experimental.pallas import tpu as pltpu
from jax.sharding import PartitionSpec as P

ITERS = 2
relaxation = 0.7
LANES = 128
SUB = 8
OUTER = 4


def times_phase(value, turn, size, sign):
    if value is None:
        return None
    re, im = value
    turn = (sign * turn) % size
    eighth = 8 * turn
    if eighth == 0:
        return value
    if eighth == 2 * size:
        return (-im, re)
    if eighth == 4 * size:
        return (-re, -im)
    if eighth == 6 * size:
        return (im, -re)
    angle = 2.0 * math.pi * turn / size
    cosine, sine = math.cos(angle), math.sin(angle)
    if eighth % size == 0:
        root = math.sqrt(0.5)
        first, second = (re - im) * root, (re + im) * root
        if eighth == size:
            return (first, second)
        if eighth == 3 * size:
            return (-second, first)
        if eighth == 5 * size:
            return (-first, -second)
        return (second, -first)
    return (re * cosine - im * sine, re * sine + im * cosine)


def plus(a, b):
    if a is None:
        return b
    if b is None:
        return a
    return (a[0] + b[0], a[1] + b[1])


def minus(a, b):
    if b is None:
        return a
    if a is None:
        return (-b[0], -b[1])
    return (a[0] - b[0], a[1] - b[1])


def transform(values, sign, wanted):
    size = len(values)
    if all(v is None for v in values):
        return [None] * wanted
    if size == 1:
        return list(values)
    half = size // 2
    if size % 2:
        raise ValueError("length")
    even = transform(values[0::2], sign, min(half, wanted))
    odd = transform(values[1::2], sign, min(half, wanted))
    odd = [times_phase(v, k, size, sign) for k, v in enumerate(odd)]
    low = [plus(a, b) for a, b in zip(even, odd)]
    high = [minus(a, b) for a, b in zip(even, odd)]
    return (low + high)[:wanted]


def tables(depth, width):
    half = width // 2
    length = depth + 2 * half
    count = length // 2 + 1
    k = np.arange(count)
    field = np.zeros((depth, 2 * LANES))
    turns = (np.arange(depth)[:, None] + half) * k[None, :] % length
    angle = turns * (2.0 * np.pi / length)
    field[:, :count] = np.cos(angle)
    field[:, LANES : LANES + count] = -np.sin(angle)
    kernel = np.zeros((LANES, 2 * LANES))
    angle = np.arange(width)[:, None] * k[None, :] % length * (2.0 * np.pi / length)
    kernel[:width, :count] = np.cos(angle)
    kernel[:width, LANES : LANES + count] = np.sin(angle)
    back = np.zeros((2 * LANES, depth))
    weight = np.where((k == 0) | (2 * k == length), 1.0, 2.0) / length
    angle = k[:, None] * np.arange(depth)[None, :] % length * (2.0 * np.pi / length)
    back[:count] = weight[:, None] * np.cos(angle)
    back[LANES : LANES + count] = -weight[:, None] * np.sin(angle)
    return field, kernel, back


def stacked(table):
    high = jnp.asarray(table, jnp.float32).astype(jnp.bfloat16)
    low = (jnp.asarray(table, jnp.float32) - high.astype(jnp.float32)).astype(jnp.bfloat16)
    return jnp.concatenate([high, high, low])


def product(left, table):
    high = left.astype(jnp.bfloat16)
    low = (left - high.astype(jnp.float32)).astype(jnp.bfloat16)
    left = jnp.concatenate([high, low, high], axis=1)
    rows = left.shape[0]
    cut = rows // 2 // (2 * SUB) * (2 * SUB) if rows >= 2 * LANES else 0
    dot = lambda part: jnp.dot(part, table, preferred_element_type=jnp.float32)
    return jnp.concatenate([dot(left[:cut]), dot(left[cut:])]) if cut else dot(left)


def first_pass(load, keep, size, sign):
    inner = size // OUTER
    for r in range(OUTER):
        values = transform([load(OUTER * a + r) for a in range(inner)], sign, inner)
        for m, value in enumerate(values):
            keep(r * inner + m, times_phase(value, r * m, size, sign))


def second_pass(kept, size, sign, wanted):
    inner = size // OUTER
    for m in range(inner):
        values = [kept(r * inner + m) for r in range(OUTER)]
        for q, value in enumerate(transform(values, sign, wanted // inner)):
            yield m + inner * q, value


def keeper(buffer, slot):
    def keep(n, value):
        buffer[slot, 0, n], buffer[slot, 1, n] = value

    def kept(n):
        return buffer[slot, 0, n], buffer[slot, 1, n]

    return keep, kept


def rows_of(count, width):
    return -(-count * width // SUB) * SUB


def row_of(count, width, node, b):
    full = width - 1
    return node * full + b if b < full else count * full + node


def spectra(count, width, region_x, region_y, first, packed, table_ref, g_ref, k1, k2, left, work, between):
    per, rows = LANES // width, rows_of(count, width)
    for a in range(width):
        shifted = packed[a // per, pl.ds(0, rows), :]
        if a % per:
            shifted = pltpu.roll(shifted, LANES - width * (a % per), axis=1)
        left[pl.ds(a * rows, rows), :] = shifted
    both = product(left[pl.ds(0, width * rows), :], table_ref[...])
    k1[0, pl.ds(0, width * rows), :] = both[:, :LANES]
    k1[1, pl.ds(0, width * rows), :] = both[:, LANES:]

    @pl.loop(0, rows // SUB)
    def _(tile):
        at = lambda i: pl.ds(pl.multiple_of(i * rows + tile * SUB, SUB), SUB)
        load = lambda a: (k1[0, at(a), :], k1[1, at(a), :]) if a < width else None
        keep, kept = keeper(work, 0)
        first_pass(load, keep, region_x, 1)
        for kx, (re, im) in second_pass(kept, region_x, 1, region_x):
            k2[0, at(kx), :] = re
            k2[1, at(kx), :] = im

    between()
    for node in range(count):
        @pl.loop(0, region_x // SUB)
        def _(tile):
            def load(b):
                if b >= width:
                    return None
                row = row_of(count, width, node, b)
                at = pl.ds(tile * SUB * rows + row, SUB, stride=rows)
                return k2[0, at, :], k2[1, at, :]

            keep, kept = keeper(work, 0)
            first_pass(load, keep, region_y, 1)
            for ky, (re, im) in second_pass(kept, region_y, 1, region_y):
                to = pl.ds(pl.multiple_of(ky * region_x + tile * SUB, SUB), SUB)
                g_ref[first + node, 0, to, :] = re
                g_ref[first + node, 1, to, :] = im


def halo_terms(half, count_y):
    terms = []
    for y in range(half):
        terms += [(y, y + b, b) for b in range(half - y)]
    for y in range(count_y - half, count_y):
        first = half + count_y
        terms += [(y, n, n - y) for n in range(first, y + 2 * half + 1)]
    return terms


def blend_kernels(half, count_x, count_y, places, kb):
    region_x, region_y = count_x + 2 * half, count_y + 2 * half
    width = 2 * half + 1
    terms = halo_terms(half, count_y)

    @pl.loop(0, region_x // SUB)
    def _(tile):
        for i in range(2):
            def kernel(j, b):
                ref, count, node = places[2 * j + i]
                rows = rows_of(count, width)
                at = pl.ds(tile * SUB * rows + row_of(count, width, node, b), SUB, stride=rows)
                return ref[0, at, :], ref[1, at, :]

            for b in range(width):
                mine = [(n, y) for n, (y, _, lag) in enumerate(terms) if lag == b]
                if not mine:
                    continue
                (ar, ai), (br, bi) = kernel(0, b), kernel(1, b)
                for n, y in mine:
                    t = (y + 0.5) / count_y
                    low, high = region_y * (1.0 - t), region_y * t
                    kb[i, tile, n, 0] = low * ar + high * br
                    kb[i, tile, n, 1] = low * ai + high * bi


def add_halo(half, count_x, count_y, pitch, c, kb, u):
    region_x, region_y = count_x + 2 * half, count_y + 2 * half
    terms = list(enumerate(halo_terms(half, count_y)))

    @pl.loop(0, region_x // SUB)
    def _(tile):
        for side in (range(half), range(half + count_y, region_y)):
            halo = {}
            for n in side:
                at = pl.ds(tile * SUB * pitch + n, SUB, stride=pitch)
                halo[n] = c[0, at, :], c[1, at, :]
            for i in range(2):
                for y in range(count_y):
                    mine = [(k, n) for k, (to, n, _) in terms if to == y and n in halo]
                    if not mine:
                        continue
                    at = pl.ds(pl.multiple_of(y * pitch + tile * SUB, SUB), SUB)
                    re, im = u[i, 0, at, :], u[i, 1, at, :]
                    for k, n in mine:
                        kr, ki = kb[i, tile, k, 0], kb[i, tile, k, 1]
                        vr, vi = halo[n]
                        re = re + (vr * kr - vi * ki)
                        im = im + (vr * ki + vi * kr)
                    u[i, 0, at, :] = re
                    u[i, 1, at, :] = im


def depth_forward(region, boxes, field_ref, z):
    region_y = region.shape[1]
    parts = [
        region[pl.ds(x, nx), pl.ds(y, ny), :].reshape(nx * ny, LANES) for x, nx, y, ny in boxes
    ]
    both, done = product(jnp.concatenate(parts), field_ref[...]), 0
    for x, nx, y, ny in boxes:
        for i in range(nx):
            to = pl.ds(pl.multiple_of((x + i) * region_y + y, SUB), ny)
            z[0, to, :] = both[done : done + ny, :LANES]
            z[1, to, :] = both[done : done + ny, LANES:]
            done += ny


def inline_forward(tile, region_x, region_y, pitch, z, c, work):
    def load(x):
        at = pl.ds(pl.multiple_of(x * region_y + tile * SUB, SUB), SUB)
        return z[0, at, :], z[1, at, :]

    keep, kept = keeper(work, 0)
    first_pass(load, keep, region_x, -1)
    for kx, (re, im) in second_pass(kept, region_x, -1, region_x):
        to = pl.ds(pl.multiple_of(kx * pitch + tile * SUB, SUB), SUB)
        c[0, to, :] = re
        c[1, to, :] = im


def crossline(present, nodes, count_y, region_x, region_y, pitch, g_ref, c, v, u, work):
    more = nodes[0] > 0

    @pl.loop(0, region_x // SUB)
    def _(tile):
        def load(y):
            if y not in present:
                return None
            at = pl.ds(tile * SUB * pitch + y, SUB, stride=pitch)
            return c[0, at, :], c[1, at, :]

        if not more:
            keep, kept = keeper(work, 0)
            first_pass(load, keep, region_y, -1)
            for ky, (re, im) in second_pass(kept, region_y, -1, region_y):
                v[tile, 0, ky] = re
                v[tile, 1, ky] = im

        @pl.loop(0, 2)
        def _(i):
            for j in nodes:
                def load(ky):
                    at = pl.ds(pl.multiple_of(ky * region_x + tile * SUB, SUB), SUB)
                    gr, gi = g_ref[2 * j + i, 0, at, :], g_ref[2 * j + i, 1, at, :]
                    vr, vi = v[tile, 0, ky], v[tile, 1, ky]
                    return vr * gr - vi * gi, vr * gi + vi * gr

                keep, _ = keeper(work, j)
                first_pass(load, keep, region_y, 1)
            passes = [second_pass(keeper(work, j)[1], region_y, 1, count_y) for j in nodes]
            for found in zip(*passes):
                y = found[0][0]
                to = pl.ds(pl.multiple_of(y * pitch + tile * SUB, SUB), SUB)
                parts = [(u[i, 0, to, :], u[i, 1, to, :])] if more else []
                for j, (_, (re, im)) in zip(nodes, found):
                    t = (y + 0.5) / count_y
                    weight = t if j else 1.0 - t
                    parts.append((weight * re, weight * im))
                re, im = functools.reduce(plus, parts)
                u[i, 0, to, :] = re
                u[i, 1, to, :] = im


def inline_back(tile, count_x, region_x, pitch, u, w, work):
    for i in range(2):
        def load(kx):
            at = pl.ds(tile * SUB * pitch + kx, SUB, stride=pitch)
            return u[i, 0, at, :], u[i, 1, at, :]

        keep, _ = keeper(work, i)
        first_pass(load, keep, region_x, 1)
    passes = [second_pass(keeper(work, i)[1], region_x, 1, count_x) for i in range(2)]
    for (x, (ar, ai)), (_, (br, bi)) in zip(*passes):
        s = (x + 0.5) / count_x
        w[tile, pl.ds(x * SUB, SUB), :LANES] = (1.0 - s) * ar + s * br
        w[tile, pl.ds(x * SUB, SUB), LANES:] = (1.0 - s) * ai + s * bi


class Link:
    def __init__(self, sems, k, src, dst, only=True, **by):
        self.sends, self.gets, there = only, only, {}
        for axis, step in by.items():
            here, size = lax.axis_index(axis), lax.axis_size(axis)
            inside = lambda i: jnp.logical_and(i >= 0, i < size)
            self.sends = jnp.logical_and(self.sends, inside(here + step))
            self.gets = jnp.logical_and(self.gets, inside(here - step))
            there[axis] = here + step
        self.copy = pltpu.make_async_remote_copy(
            src_ref=src, dst_ref=dst, send_sem=sems[0].at[k], recv_sem=sems[1].at[k],
            device_id=there, device_id_type=pl.DeviceIdType.MESH,
        )

    def start(self):
        pl.when(self.sends)(lambda: self.copy.start())

    def wait_recv(self):
        pl.when(self.gets)(lambda: self.copy.wait_recv())

    def wait_send(self):
        pl.when(self.sends)(lambda: self.copy.wait_send())


LINKS = 12


def halo_links(region, count_x, count_y, half, sems, base, direct):
    gx, gy, size = lax.axis_index("gx"), lax.axis_index("gy"), lax.axis_size("gy")
    low, high_x, high_y = pl.ds(0, half), pl.ds(half + count_x, half), pl.ds(half + count_y, half)
    last_x, last_y, first = pl.ds(count_x, half), pl.ds(count_y, half), pl.ds(half, half)
    at = lambda x, y: region.at[x, y]
    part_x, part_y = count_x // 2, count_y // 2
    along_y = []
    for n, (src, dst, by) in enumerate(((first, high_y, -1), (last_y, low, 1))):
        along_y.append([])
        for k in range(2):
            x = pl.ds(half + part_x * ((gx + 1 + k) % 2), part_x)
            along_y[n].append(Link(sems, base + 2 * n + k, at(x, src), at(x, dst), gy=by))
    along_x = []
    for n in range(2):
        part = pl.ds(half + n * part_y, part_y)
        along_x.append([
            Link(sems, base + 4 + 2 * n, at(last_x, part), at(low, part), gx=1),
            Link(sems, base + 5 + 2 * n, at(first, part), at(high_x, part), gx=-1),
        ])
    relayed = []
    sides = ((high_y, first, -1, gy < size - 1), (low, last_y, 1, gy > 0))
    for n, (dst, src, by, has) in enumerate(sides):
        if direct:
            up = Link(sems, base + 8 + 2 * n, at(low, src), at(low, dst), gx > 0, gy=by)
        else:
            up = Link(sems, base + 8 + 2 * n, at(last_x, dst), at(low, dst), has, gx=1)
        down = Link(sems, base + 9 + 2 * n, at(first, dst), at(high_x, dst), has, gx=-1)
        relayed.append([up, down])
    return along_y, along_x, relayed


def whole_kernel(
    count_x, count_y, half, pitch,
    data_hbm, precond_hbm, psf_hbm, field_hbm, kernel_hbm, back_hbm,
    model_ref, residual_ref,
    data_ref, precond_ref, psf_ref, field_ref, kernel_ref, back_ref,
    region0, region1, wide, nodes, packed, left, g_ref, k1, k2a, k2b, k2c, kb, z, c, v, u, w, work,
    load_sem, send_sem, recv_sem,
):
    width = 2 * half + 1
    full = width - 1
    per = LANES // width
    region_x, region_y = count_x + 2 * half, count_y + 2 * half
    sems = (send_sem, recv_sem)
    gx, gy = lax.axis_index("gx"), lax.axis_index("gy")
    size_x, size_y = lax.axis_size("gx"), lax.axis_size("gy")
    regions = [region0, region1]

    barrier = pltpu.get_barrier_semaphore()
    for axis, here, size in (("gx", gx, size_x), ("gy", gy, size_y)):
        for by in (-1, 1):
            @pl.when(jnp.logical_and(here + by >= 0, here + by < size))
            def _():
                pl.semaphore_signal(
                    barrier, inc=1, device_id={axis: here + by},
                    device_id_type=pl.DeviceIdType.MESH,
                )

    pairs = [
        (psf_hbm.at[:, :, 0, :], psf_ref), (data_hbm, data_ref), (precond_hbm, precond_ref),
        (kernel_hbm, kernel_ref), (field_hbm, field_ref), (back_hbm, back_ref),
    ]
    loads = [pltpu.make_async_copy(a, b, load_sem.at[k]) for k, (a, b) in enumerate(pairs)]
    for load in loads:
        load.start()

    wide[...] = jnp.zeros(wide.shape, wide.dtype)
    packed[...] = jnp.zeros(packed.shape, packed.dtype)
    every = slice(None)
    edges = [
        (gx == 0, (pl.ds(0, half), every)), (gx == size_x - 1, (pl.ds(half + count_x, half), every)),
        (gy == 0, (every, pl.ds(0, half))), (gy == size_y - 1, (every, pl.ds(half + count_y, half))),
    ]
    for edge, at in edges:
        @pl.when(edge)
        def _():
            for region in regions:
                region[at] = jnp.zeros(region[at].shape, region.dtype)

    loads[0].wait()
    for a in range(width):
        wide[a, pl.ds(0, width), pl.ds(0, width)] = psf_ref[a]
    for n in range(nodes.shape[1]):
        total = wide[n * per]
        for a in range(n * per + 1, min(width, (n + 1) * per)):
            total = total + pltpu.roll(wide[a], width * (a % per), axis=1)
        nodes[0, n] = total
    loads[1].wait()
    loads[2].wait()
    own = (pl.ds(half, count_x), pl.ds(half, count_y))
    region0[own] = precond_ref[...] * data_ref[...]

    peers = 0
    for here, size in ((gx, size_x), (gy, size_y)):
        peers += (here > 0).astype(jnp.int32) + (here < size - 1).astype(jnp.int32)
    pl.semaphore_wait(barrier, peers)

    inline = Link(sems, 0, nodes.at[0], nodes.at[1], gx=-1)
    cross = Link(sems, 1, nodes.at[0], nodes.at[2], gy=-1)
    corner = Link(sems, 2, nodes.at[2], nodes.at[3], gy < size_y - 1, gx=-1)
    cross.start()
    inline.start()
    started = [cross, inline, corner]
    last_x, last_y = gx == size_x - 1, gy == size_y - 1
    links = [
        halo_links(regions[n], count_x, count_y, half, sems, 3 + LINKS * n, n > 0)
        for n in range(ITERS)
    ]
    for along_y, along_x, relayed in links:
        started += sum(along_y + along_x + relayed, [])

    def send(links):
        for link in links:
            link.start()

    def pack(count, place, node):
        packed[:, pl.ds(place * full, full), :] = nodes[node, :, pl.ds(0, full), :]
        packed[:, pl.ds(count * full + place, 1), :] = nodes[node, :, pl.ds(full, 1), :]

    def node_spectra(count, first, k2, between=lambda: None):
        spectra(
            count, width, region_x, region_y, first, packed, kernel_ref, g_ref, k1, k2, left, work,
            between,
        )

    def inline_tiles(count, tile_of):
        @pl.loop(0, count)
        def _(n):
            inline_forward(tile_of(n), region_x, region_y, pitch, z, c, work)

    def own_forward(region, along_x, after=()):
        depth_forward(region, [(half, count_x, half, count_y)], field_ref, z)
        for link in along_x[0] + along_x[1]:
            link.wait_recv()
        send(after)
        sides = [(x, half, half, count_y) for x in (0, half + count_x)]
        depth_forward(region, sides, field_ref, z)
        inline_tiles(count_y // SUB, lambda n: n + half // SUB)

    def relay(along_y, relayed, k, direct=False):
        for n in range(2):
            along_y[n][k].wait_recv()
            for parity in range(int(direct), 2):
                pl.when((gx + k) % 2 == parity)(relayed[n][parity].start)

    def half_boxes(k):
        x = half + count_x // 2 * ((gx + 1 + k) % 2)
        return [(x, count_x // 2, y, half) for y in (0, half + count_y)]

    def halo_forward(region, along_y, relayed, direct):
        if direct:
            relay(along_y, relayed, 0, True)
        depth_forward(region, half_boxes(0), field_ref, z)
        relay(along_y, relayed, 1, direct)
        for link in relayed[0] + relayed[1]:
            link.wait_recv()
        corners = [
            (x, half, y, half) for x in (0, half + count_x) for y in (0, half + count_y)
        ]
        depth_forward(region, half_boxes(1) + corners, field_ref, z)
        edge, skip = half // SUB, count_y // SUB
        inline_tiles(2 * edge, lambda n: n + (n // edge) * skip)

    def operator(*nodes):
        own = range(half, half + count_y)
        crossline(own, nodes, count_y, region_x, region_y, pitch, g_ref, c, v, u, work)

    def finish(sweep_index):
        region, last = regions[sweep_index], sweep_index == ITERS - 1
        tiles = count_y // SUB

        @pl.loop(0, tiles)
        def _(tile):
            inline_back(tile, count_x, region_x, pitch, u, w, work)

        rows = count_x * SUB
        blended = product(w[...].reshape(tiles * rows, 2 * LANES), back_ref[...])
        for tile in range(tiles):
            here = pl.ds(tile * SUB, SUB)
            inner = pl.ds(half + tile * SUB, SUB)
            for x in range(count_x):
                at = tile * rows + x * SUB
                model = region[x + half, inner, :]
                residual = data_ref[x, here, :] - (model + blended[at : at + SUB])
                model = model + relaxation * precond_ref[x, here, :] * residual
                if last:
                    residual_ref[x, here, :] = residual
                    model_ref[x, here, :] = model
                else:
                    regions[sweep_index + 1][x + half, inner, :] = model
        if not last:
            along_y, along_x, _ = links[sweep_index + 1]
            send(along_x[0] + along_x[1])
            send([along_y[0][0], along_y[1][0], along_y[0][1], along_y[1][1]])

    along_y, along_x, relayed = links[0]
    send(along_x[0] + along_x[1])
    send([along_y[0][0], along_y[1][0], along_y[0][1], along_y[1][1]])
    loads[3].wait()
    pack(2, 0, 0)
    inline.wait_recv()
    pl.when(last_x)(lambda: pack(2, 1, 0))
    pl.when(jnp.logical_not(last_x))(lambda: pack(2, 1, 1))
    node_spectra(2, 0, k2a)
    loads[4].wait()
    loads[5].wait()
    own_forward(region0, along_x)
    operator(0)
    cross.wait_recv()
    corner.start()
    pl.when(last_y)(lambda: pack(1, 0, 0))
    pl.when(jnp.logical_not(last_y))(lambda: pack(1, 0, 2))
    node_spectra(1, 2, k2b)
    corner.wait_recv()
    for edge_x in (False, True):
        for edge_y in (False, True):
            here = (last_x if edge_x else jnp.logical_not(last_x),
                    last_y if edge_y else jnp.logical_not(last_y))
            source = (0 if edge_y else 2) if edge_x else (1 if edge_y else 3)
            pl.when(jnp.logical_and(*here))(lambda: pack(1, 0, source))
    node_spectra(1, 3, k2c, lambda: relay(along_y, relayed, 0))
    operator(1)
    places = [(k2a, 2, 0), (k2a, 2, 1), (k2b, 1, 0), (k2c, 1, 0)]
    blend_kernels(half, count_x, count_y, places, kb)
    halo_forward(region0, along_y, relayed, False)
    add_halo(half, count_x, count_y, pitch, c, kb, u)
    finish(0)
    for sweep_index in range(1, ITERS):
        region = regions[sweep_index]
        along_y, along_x, relayed = links[sweep_index]
        own_forward(region, along_x, [relayed[0][0], relayed[1][0]])
        operator(0, 1)
        halo_forward(region, along_y, relayed, True)
        add_halo(half, count_x, count_y, pitch, c, kb, u)
        finish(sweep_index)
    for link in started:
        link.wait_send()


def local(data, precond, psf):
    count_x, count_y, depth = data.shape
    width = psf.shape[2]
    half = width // 2
    region_x, region_y = count_x + 2 * half, count_y + 2 * half
    field, kernel, back = tables(depth, width)
    back = back / (region_x * region_y)
    f32 = jnp.float32
    up = lambda n, m: -(-n // m) * m
    high, columns = up(width, SUB), up(width, LANES // width) // (LANES // width)
    rows, single = rows_of(2, width), rows_of(1, width)
    terms = len(halo_terms(half, count_y))
    pitch = max(region_x, region_y) + SUB
    vmem = lambda *shape: pltpu.VMEM(shape, f32)
    table = lambda *shape: pltpu.VMEM(shape, jnp.bfloat16)
    square = region_x * region_y
    flat = psf.transpose(0, 2, 3, 1, 4).reshape(width, width, 1, width)
    operands = (data, precond, flat, stacked(field), stacked(kernel), stacked(back))
    model, residual = pl.pallas_call(
        functools.partial(whole_kernel, count_x, count_y, half, pitch),
        out_shape=[jax.ShapeDtypeStruct(data.shape, f32)] * 2,
        in_specs=[pl.BlockSpec(memory_space=pltpu.HBM)] * 6,
        out_specs=[pl.BlockSpec(memory_space=pltpu.VMEM)] * 2,
        scratch_shapes=[
            vmem(*data.shape),
            vmem(*data.shape),
            vmem(width, width, width),
            table(*operands[3].shape),
            table(*operands[4].shape),
            table(*operands[5].shape),
            vmem(region_x, region_y, depth),
            vmem(region_x, region_y, depth),
            vmem(width, high, LANES),
            vmem(4, columns, high, LANES),
            vmem(columns, rows, LANES),
            vmem(width * rows, LANES),
            vmem(4, 2, square, LANES),
            vmem(2, width * rows, LANES),
            vmem(2, region_x * rows, LANES),
            vmem(2, region_x * single, LANES),
            vmem(2, region_x * single, LANES),
            vmem(2, region_x // SUB, terms, 2, SUB, LANES),
            vmem(2, square, LANES),
            vmem(2, region_x * pitch, LANES),
            vmem(region_x // SUB, 2, region_y, SUB, LANES),
            vmem(2, 2, count_y * pitch, LANES),
            vmem(count_y // SUB, count_x * SUB, 2 * LANES),
            vmem(2, 2, max(region_x, region_y), SUB, LANES),
            pltpu.SemaphoreType.DMA((6,)),
            pltpu.SemaphoreType.DMA((3 + LINKS * ITERS,)),
            pltpu.SemaphoreType.DMA((3 + LINKS * ITERS,)),
        ],
        compiler_params=pltpu.CompilerParams(
            vmem_limit_bytes=54976 << 10, collective_id=0, has_side_effects=True
        ),
        name="whole",
    )(*operands)
    def tail(a, b, c, e, sems):
        copies = [pltpu.make_async_copy(a, c, sems.at[0]), pltpu.make_async_copy(b, e, sems.at[1])]
        for copy in copies:
            copy.start()
        for copy in copies:
            copy.wait()

    return pl.pallas_call(
        tail,
        out_shape=[jax.ShapeDtypeStruct(data.shape, f32)] * 2,
        in_specs=[pl.BlockSpec(memory_space=pltpu.VMEM)] * 2,
        out_specs=[pl.BlockSpec(memory_space=pl.ANY)] * 2,
        scratch_shapes=[pltpu.SemaphoreType.DMA((2,))],
        compiler_params=pltpu.CompilerParams(vmem_limit_bytes=54976 << 10),
        name="tail",
    )(model, residual)


def solution(mesh):
    placed = (P("gx", "gy", None), P("gx", "gy", None), P("gx", "gy", None, None, None))
    return jax.shard_map(
        local,
        mesh=mesh,
        in_specs=placed,
        out_specs=(P("gx", "gy", None), P("gx", "gy", None)),
        check_vma=False,
    )
```

```python
import functools
import math

import jax
import jax.numpy as jnp
import numpy as np
from jax import lax
from jax.experimental import pallas as pl
from jax.experimental.pallas import tpu as pltpu
from jax.sharding import PartitionSpec as P

ITERS = 2
relaxation = 0.7
LANES = 128
SUB = 8
OUTER = 4


def times_phase(value, turn, size, sign):
    if value is None:
        return None
    re, im = value
    turn = (sign * turn) % size
    eighth = 8 * turn
    if eighth == 0:
        return value
    if eighth == 2 * size:
        return (-im, re)
    if eighth == 4 * size:
        return (-re, -im)
    if eighth == 6 * size:
        return (im, -re)
    angle = 2.0 * math.pi * turn / size
    cosine, sine = math.cos(angle), math.sin(angle)
    if eighth % size == 0:
        root = math.sqrt(0.5)
        first, second = (re - im) * root, (re + im) * root
        if eighth == size:
            return (first, second)
        if eighth == 3 * size:
            return (-second, first)
        if eighth == 5 * size:
            return (-first, -second)
        return (second, -first)
    return (re * cosine - im * sine, re * sine + im * cosine)


def plus(a, b):
    if a is None:
        return b
    if b is None:
        return a
    return (a[0] + b[0], a[1] + b[1])


def minus(a, b):
    if b is None:
        return a
    if a is None:
        return (-b[0], -b[1])
    return (a[0] - b[0], a[1] - b[1])


def transform(values, sign, wanted):
    size = len(values)
    if all(v is None for v in values):
        return [None] * wanted
    if size == 1:
        return list(values)
    half = size // 2
    if size % 2:
        raise ValueError("length")
    even = transform(values[0::2], sign, min(half, wanted))
    odd = transform(values[1::2], sign, min(half, wanted))
    odd = [times_phase(v, k, size, sign) for k, v in enumerate(odd)]
    low = [plus(a, b) for a, b in zip(even, odd)]
    high = [minus(a, b) for a, b in zip(even, odd)]
    return (low + high)[:wanted]


def tables(depth, width):
    half = width // 2
    length = depth + 2 * half
    count = length // 2 + 1
    k = np.arange(count)
    field = np.zeros((depth, 2 * LANES))
    turns = (np.arange(depth)[:, None] + half) * k[None, :] % length
    angle = turns * (2.0 * np.pi / length)
    field[:, :count] = np.cos(angle)
    field[:, LANES : LANES + count] = -np.sin(angle)
    kernel = np.zeros((LANES, 2 * LANES))
    angle = np.arange(width)[:, None] * k[None, :] % length * (2.0 * np.pi / length)
    kernel[:width, :count] = np.cos(angle)
    kernel[:width, LANES : LANES + count] = np.sin(angle)
    back = np.zeros((2 * LANES, depth))
    weight = np.where((k == 0) | (2 * k == length), 1.0, 2.0) / length
    angle = k[:, None] * np.arange(depth)[None, :] % length * (2.0 * np.pi / length)
    back[:count] = weight[:, None] * np.cos(angle)
    back[LANES : LANES + count] = -weight[:, None] * np.sin(angle)
    return field, kernel, back


def stacked(table):
    high = jnp.asarray(table, jnp.float32).astype(jnp.bfloat16)
    low = (jnp.asarray(table, jnp.float32) - high.astype(jnp.float32)).astype(jnp.bfloat16)
    return jnp.concatenate([high, high, low])


def product(left, table):
    high = left.astype(jnp.bfloat16)
    low = (left - high.astype(jnp.float32)).astype(jnp.bfloat16)
    left = jnp.concatenate([high, low, high], axis=1)
    rows = left.shape[0]
    cut = rows // 2 // (2 * SUB) * (2 * SUB) if rows >= 2 * LANES else 0
    dot = lambda part: jnp.dot(part, table, preferred_element_type=jnp.float32)
    return jnp.concatenate([dot(left[:cut]), dot(left[cut:])]) if cut else dot(left)


def first_pass(load, keep, size, sign):
    inner = size // OUTER
    for r in range(OUTER):
        values = transform([load(OUTER * a + r) for a in range(inner)], sign, inner)
        for m, value in enumerate(values):
            keep(r * inner + m, times_phase(value, r * m, size, sign))


def second_pass(kept, size, sign, wanted):
    inner = size // OUTER
    for m in range(inner):
        values = [kept(r * inner + m) for r in range(OUTER)]
        for q, value in enumerate(transform(values, sign, wanted // inner)):
            yield m + inner * q, value


def keeper(buffer, slot):
    def keep(n, value):
        buffer[slot, 0, n], buffer[slot, 1, n] = value

    def kept(n):
        return buffer[slot, 0, n], buffer[slot, 1, n]

    return keep, kept


def rows_of(count, width):
    return -(-count * width // SUB) * SUB


def row_of(count, width, node, b):
    full = width - 1
    return node * full + b if b < full else count * full + node


def spectra(count, width, region_x, region_y, first, packed, table_ref, g_ref, k1, k2, left, work, between):
    per, rows = LANES // width, rows_of(count, width)
    for a in range(width):
        shifted = packed[a // per, pl.ds(0, rows), :]
        if a % per:
            shifted = pltpu.roll(shifted, LANES - width * (a % per), axis=1)
        left[pl.ds(a * rows, rows), :] = shifted
    both = product(left[pl.ds(0, width * rows), :], table_ref[...])
    k1[0, pl.ds(0, width * rows), :] = both[:, :LANES]
    k1[1, pl.ds(0, width * rows), :] = both[:, LANES:]

    @pl.loop(0, rows // SUB)
    def _(tile):
        at = lambda i: pl.ds(pl.multiple_of(i * rows + tile * SUB, SUB), SUB)
        load = lambda a: (k1[0, at(a), :], k1[1, at(a), :]) if a < width else None
        keep, kept = keeper(work, 0)
        first_pass(load, keep, region_x, 1)
        for kx, (re, im) in second_pass(kept, region_x, 1, region_x):
            k2[0, at(kx), :] = re
            k2[1, at(kx), :] = im

    between()
    for node in range(count):
        @pl.loop(0, region_x // SUB)
        def _(tile):
            def load(b):
                if b >= width:
                    return None
                row = row_of(count, width, node, b)
                at = pl.ds(tile * SUB * rows + row, SUB, stride=rows)
                return k2[0, at, :], k2[1, at, :]

            keep, kept = keeper(work, 0)
            first_pass(load, keep, region_y, 1)
            for ky, (re, im) in second_pass(kept, region_y, 1, region_y):
                to = pl.ds(pl.multiple_of(ky * region_x + tile * SUB, SUB), SUB)
                g_ref[first + node, 0, to, :] = re
                g_ref[first + node, 1, to, :] = im


def halo_terms(half, count_y):
    terms = []
    for y in range(half):
        terms += [(y, y + b, b) for b in range(half - y)]
    for y in range(count_y - half, count_y):
        first = half + count_y
        terms += [(y, n, n - y) for n in range(first, y + 2 * half + 1)]
    return terms


def blend_kernels(half, count_x, count_y, places, kb):
    region_x, region_y = count_x + 2 * half, count_y + 2 * half
    width = 2 * half + 1
    terms = halo_terms(half, count_y)

    @pl.loop(0, region_x // SUB)
    def _(tile):
        for i in range(2):
            def kernel(j, b):
                ref, count, node = places[2 * j + i]
                rows = rows_of(count, width)
                at = pl.ds(tile * SUB * rows + row_of(count, width, node, b), SUB, stride=rows)
                return ref[0, at, :], ref[1, at, :]

            for b in range(width):
                mine = [(n, y) for n, (y, _, lag) in enumerate(terms) if lag == b]
                if not mine:
                    continue
                (ar, ai), (br, bi) = kernel(0, b), kernel(1, b)
                for n, y in mine:
                    t = (y + 0.5) / count_y
                    low, high = region_y * (1.0 - t), region_y * t
                    kb[i, tile, n, 0] = low * ar + high * br
                    kb[i, tile, n, 1] = low * ai + high * bi


def add_halo(half, count_x, count_y, pitch, c, kb, u):
    region_x, region_y = count_x + 2 * half, count_y + 2 * half
    terms = list(enumerate(halo_terms(half, count_y)))

    @pl.loop(0, region_x // SUB)
    def _(tile):
        for side in (range(half), range(half + count_y, region_y)):
            halo = {}
            for n in side:
                at = pl.ds(tile * SUB * pitch + n, SUB, stride=pitch)
                halo[n] = c[0, at, :], c[1, at, :]
            for i in range(2):
                for y in range(count_y):
                    mine = [(k, n) for k, (to, n, _) in terms if to == y and n in halo]
                    if not mine:
                        continue
                    at = pl.ds(pl.multiple_of(y * pitch + tile * SUB, SUB), SUB)
                    re, im = u[i, 0, at, :], u[i, 1, at, :]
                    for k, n in mine:
                        kr, ki = kb[i, tile, k, 0], kb[i, tile, k, 1]
                        vr, vi = halo[n]
                        re = re + (vr * kr - vi * ki)
                        im = im + (vr * ki + vi * kr)
                    u[i, 0, at, :] = re
                    u[i, 1, at, :] = im


def depth_forward(region, boxes, field_ref, z):
    region_y = region.shape[1]
    parts = [
        region[pl.ds(x, nx), pl.ds(y, ny), :].reshape(nx * ny, LANES) for x, nx, y, ny in boxes
    ]
    both, done = product(jnp.concatenate(parts), field_ref[...]), 0
    for x, nx, y, ny in boxes:
        for i in range(nx):
            to = pl.ds(pl.multiple_of((x + i) * region_y + y, SUB), ny)
            z[0, to, :] = both[done : done + ny, :LANES]
            z[1, to, :] = both[done : done + ny, LANES:]
            done += ny


def inline_forward(tile, region_x, region_y, pitch, z, c, work):
    def load(x):
        at = pl.ds(pl.multiple_of(x * region_y + tile * SUB, SUB), SUB)
        return z[0, at, :], z[1, at, :]

    keep, kept = keeper(work, 0)
    first_pass(load, keep, region_x, -1)
    for kx, (re, im) in second_pass(kept, region_x, -1, region_x):
        to = pl.ds(pl.multiple_of(kx * pitch + tile * SUB, SUB), SUB)
        c[0, to, :] = re
        c[1, to, :] = im


def crossline(present, nodes, count_y, region_x, region_y, pitch, g_ref, c, v, u, work):
    more = nodes[0] > 0

    @pl.loop(0, region_x // SUB)
    def _(tile):
        def load(y):
            if y not in present:
                return None
            at = pl.ds(tile * SUB * pitch + y, SUB, stride=pitch)
            return c[0, at, :], c[1, at, :]

        if not more:
            keep, kept = keeper(work, 0)
            first_pass(load, keep, region_y, -1)
            for ky, (re, im) in second_pass(kept, region_y, -1, region_y):
                v[tile, 0, ky] = re
                v[tile, 1, ky] = im

        @pl.loop(0, 2)
        def _(i):
            for j in nodes:
                def load(ky):
                    at = pl.ds(pl.multiple_of(ky * region_x + tile * SUB, SUB), SUB)
                    gr, gi = g_ref[2 * j + i, 0, at, :], g_ref[2 * j + i, 1, at, :]
                    vr, vi = v[tile, 0, ky], v[tile, 1, ky]
                    return vr * gr - vi * gi, vr * gi + vi * gr

                keep, _ = keeper(work, j)
                first_pass(load, keep, region_y, 1)
            passes = [second_pass(keeper(work, j)[1], region_y, 1, count_y) for j in nodes]
            for found in zip(*passes):
                y = found[0][0]
                to = pl.ds(pl.multiple_of(y * pitch + tile * SUB, SUB), SUB)
                parts = [(u[i, 0, to, :], u[i, 1, to, :])] if more else []
                for j, (_, (re, im)) in zip(nodes, found):
                    t = (y + 0.5) / count_y
                    weight = t if j else 1.0 - t
                    parts.append((weight * re, weight * im))
                re, im = functools.reduce(plus, parts)
                u[i, 0, to, :] = re
                u[i, 1, to, :] = im


def inline_back(tile, count_x, region_x, pitch, u, w, work):
    for i in range(2):
        def load(kx):
            at = pl.ds(tile * SUB * pitch + kx, SUB, stride=pitch)
            return u[i, 0, at, :], u[i, 1, at, :]

        keep, _ = keeper(work, i)
        first_pass(load, keep, region_x, 1)
    passes = [second_pass(keeper(work, i)[1], region_x, 1, count_x) for i in range(2)]
    for (x, (ar, ai)), (_, (br, bi)) in zip(*passes):
        s = (x + 0.5) / count_x
        w[tile, pl.ds(x * SUB, SUB), :LANES] = (1.0 - s) * ar + s * br
        w[tile, pl.ds(x * SUB, SUB), LANES:] = (1.0 - s) * ai + s * bi


class Link:
    def __init__(self, sems, k, src, dst, only=True, **by):
        self.sends, self.gets, there = only, only, {}
        for axis, step in by.items():
            here, size = lax.axis_index(axis), lax.axis_size(axis)
            inside = lambda i: jnp.logical_and(i >= 0, i < size)
            self.sends = jnp.logical_and(self.sends, inside(here + step))
            self.gets = jnp.logical_and(self.gets, inside(here - step))
            there[axis] = here + step
        self.copy = pltpu.make_async_remote_copy(
            src_ref=src, dst_ref=dst, send_sem=sems[0].at[k], recv_sem=sems[1].at[k],
            device_id=there, device_id_type=pl.DeviceIdType.MESH,
        )

    def start(self):
        pl.when(self.sends)(lambda: self.copy.start())

    def wait_recv(self):
        pl.when(self.gets)(lambda: self.copy.wait_recv())

    def wait_send(self):
        pl.when(self.sends)(lambda: self.copy.wait_send())


LINKS = 12


def halo_links(region, count_x, count_y, half, sems, base, direct):
    gx, gy, size = lax.axis_index("gx"), lax.axis_index("gy"), lax.axis_size("gy")
    low, high_x, high_y = pl.ds(0, half), pl.ds(half + count_x, half), pl.ds(half + count_y, half)
    last_x, last_y, first = pl.ds(count_x, half), pl.ds(count_y, half), pl.ds(half, half)
    at = lambda x, y: region.at[x, y]
    part_x, part_y = count_x // 2, count_y // 2
    along_y = []
    for n, (src, dst, by) in enumerate(((first, high_y, -1), (last_y, low, 1))):
        along_y.append([])
        for k in range(2):
            x = pl.ds(half + part_x * ((gx + 1 + k) % 2), part_x)
            along_y[n].append(Link(sems, base + 2 * n + k, at(x, src), at(x, dst), gy=by))
    along_x = []
    for n in range(2):
        part = pl.ds(half + n * part_y, part_y)
        along_x.append([
            Link(sems, base + 4 + 2 * n, at(last_x, part), at(low, part), gx=1),
            Link(sems, base + 5 + 2 * n, at(first, part), at(high_x, part), gx=-1),
        ])
    relayed = []
    sides = ((high_y, first, -1, gy < size - 1), (low, last_y, 1, gy > 0))
    for n, (dst, src, by, has) in enumerate(sides):
        if direct:
            up = Link(sems, base + 8 + 2 * n, at(low, src), at(low, dst), gx > 0, gy=by)
        else:
            up = Link(sems, base + 8 + 2 * n, at(last_x, dst), at(low, dst), has, gx=1)
        down = Link(sems, base + 9 + 2 * n, at(first, dst), at(high_x, dst), has, gx=-1)
        relayed.append([up, down])
    return along_y, along_x, relayed


def whole_kernel(
    count_x, count_y, half, pitch,
    data_hbm, precond_hbm, psf_hbm, field_hbm, kernel_hbm, back_hbm,
    model_ref, residual_ref,
    data_ref, precond_ref, psf_ref, field_ref, kernel_ref, back_ref,
    region0, region1, wide, nodes, packed, left, g_ref, k1, k2a, k2b, k2c, kb, z, c, v, u, w, work,
    load_sem, send_sem, recv_sem,
):
    width = 2 * half + 1
    full = width - 1
    per = LANES // width
    region_x, region_y = count_x + 2 * half, count_y + 2 * half
    sems = (send_sem, recv_sem)
    gx, gy = lax.axis_index("gx"), lax.axis_index("gy")
    size_x, size_y = lax.axis_size("gx"), lax.axis_size("gy")
    regions = [region0, region1]

    barrier = pltpu.get_barrier_semaphore()
    for axis, here, size in (("gx", gx, size_x), ("gy", gy, size_y)):
        for by in (-1, 1):
            @pl.when(jnp.logical_and(here + by >= 0, here + by < size))
            def _():
                pl.semaphore_signal(
                    barrier, inc=1, device_id={axis: here + by},
                    device_id_type=pl.DeviceIdType.MESH,
                )

    pairs = [
        (psf_hbm.at[:, :, 0, :], psf_ref), (data_hbm, data_ref), (precond_hbm, precond_ref),
        (kernel_hbm, kernel_ref), (field_hbm, field_ref), (back_hbm, back_ref),
    ]
    loads = [pltpu.make_async_copy(a, b, load_sem.at[k]) for k, (a, b) in enumerate(pairs)]
    for load in loads:
        load.start()

    wide[...] = jnp.zeros(wide.shape, wide.dtype)
    packed[...] = jnp.zeros(packed.shape, packed.dtype)
    every = slice(None)
    edges = [
        (gx == 0, (pl.ds(0, half), every)), (gx == size_x - 1, (pl.ds(half + count_x, half), every)),
        (gy == 0, (every, pl.ds(0, half))), (gy == size_y - 1, (every, pl.ds(half + count_y, half))),
    ]
    for edge, at in edges:
        @pl.when(edge)
        def _():
            for region in regions:
                region[at] = jnp.zeros(region[at].shape, region.dtype)

    loads[0].wait()
    for a in range(width):
        wide[a, pl.ds(0, width), pl.ds(0, width)] = psf_ref[a]
    for n in range(nodes.shape[1]):
        total = wide[n * per]
        for a in range(n * per + 1, min(width, (n + 1) * per)):
            total = total + pltpu.roll(wide[a], width * (a % per), axis=1)
        nodes[0, n] = total
    loads[1].wait()
    loads[2].wait()
    own = (pl.ds(half, count_x), pl.ds(half, count_y))
    region0[own] = precond_ref[...] * data_ref[...]

    peers = 0
    for here, size in ((gx, size_x), (gy, size_y)):
        peers += (here > 0).astype(jnp.int32) + (here < size - 1).astype(jnp.int32)
    pl.semaphore_wait(barrier, peers)

    inline = Link(sems, 0, nodes.at[0], nodes.at[1], gx=-1)
    cross = Link(sems, 1, nodes.at[0], nodes.at[2], gy=-1)
    corner = Link(sems, 2, nodes.at[2], nodes.at[3], gy < size_y - 1, gx=-1)
    cross.start()
    inline.start()
    started = [cross, inline, corner]
    last_x, last_y = gx == size_x - 1, gy == size_y - 1
    links = [
        halo_links(regions[n], count_x, count_y, half, sems, 3 + LINKS * n, n > 0)
        for n in range(ITERS)
    ]
    for along_y, along_x, relayed in links:
        started += sum(along_y + along_x + relayed, [])

    def send(links):
        for link in links:
            link.start()

    def pack(count, place, node):
        packed[:, pl.ds(place * full, full), :] = nodes[node, :, pl.ds(0, full), :]
        packed[:, pl.ds(count * full + place, 1), :] = nodes[node, :, pl.ds(full, 1), :]

    def node_spectra(count, first, k2, between=lambda: None):
        spectra(
            count, width, region_x, region_y, first, packed, kernel_ref, g_ref, k1, k2, left, work,
            between,
        )

    def inline_tiles(count, tile_of):
        @pl.loop(0, count)
        def _(n):
            inline_forward(tile_of(n), region_x, region_y, pitch, z, c, work)

    def own_depth(region):
        depth_forward(region, [(half, count_x, half, count_y)], field_ref, z)

    def own_forward(region, along_x, after=()):
        for link in along_x[0] + along_x[1]:
            link.wait_recv()
        send(after)
        sides = [(x, half, half, count_y) for x in (0, half + count_x)]
        depth_forward(region, sides, field_ref, z)
        inline_tiles(count_y // SUB, lambda n: n + half // SUB)

    def relay(along_y, relayed, k, direct=False):
        for n in range(2):
            along_y[n][k].wait_recv()
            for parity in range(int(direct), 2):
                pl.when((gx + k) % 2 == parity)(relayed[n][parity].start)

    def half_boxes(k):
        x = half + count_x // 2 * ((gx + 1 + k) % 2)
        return [(x, count_x // 2, y, half) for y in (0, half + count_y)]

    def halo_forward(region, along_y, relayed, direct):
        if direct:
            relay(along_y, relayed, 0, True)
        depth_forward(region, half_boxes(0), field_ref, z)
        relay(along_y, relayed, 1, direct)
        for link in relayed[0] + relayed[1]:
            link.wait_recv()
        corners = [
            (x, half, y, half) for x in (0, half + count_x) for y in (0, half + count_y)
        ]
        depth_forward(region, half_boxes(1) + corners, field_ref, z)
        edge, skip = half // SUB, count_y // SUB
        inline_tiles(2 * edge, lambda n: n + (n // edge) * skip)

    def operator(*nodes):
        own = range(half, half + count_y)
        crossline(own, nodes, count_y, region_x, region_y, pitch, g_ref, c, v, u, work)

    def finish(sweep_index):
        region, last = regions[sweep_index], sweep_index == ITERS - 1
        tiles = count_y // SUB

        @pl.loop(0, tiles)
        def _(tile):
            inline_back(tile, count_x, region_x, pitch, u, w, work)

        rows = count_x * SUB
        blended = product(w[...].reshape(tiles * rows, 2 * LANES), back_ref[...])
        for tile in range(tiles):
            here = pl.ds(tile * SUB, SUB)
            inner = pl.ds(half + tile * SUB, SUB)
            for x in range(count_x):
                at = tile * rows + x * SUB
                model = region[x + half, inner, :]
                residual = data_ref[x, here, :] - (model + blended[at : at + SUB])
                model = model + relaxation * precond_ref[x, here, :] * residual
                if last:
                    residual_ref[x, here, :] = residual
                    model_ref[x, here, :] = model
                else:
                    regions[sweep_index + 1][x + half, inner, :] = model
        if not last:
            along_y, along_x, _ = links[sweep_index + 1]
            send(along_x[0] + along_x[1])
            send([along_y[0][0], along_y[1][0], along_y[0][1], along_y[1][1]])

    along_y, along_x, relayed = links[0]
    send(along_x[0] + along_x[1])
    send([along_y[0][0], along_y[1][0], along_y[0][1], along_y[1][1]])
    loads[3].wait()
    loads[4].wait()
    own_depth(region0)
    pack(2, 0, 0)
    inline.wait_recv()
    pl.when(last_x)(lambda: pack(2, 1, 0))
    pl.when(jnp.logical_not(last_x))(lambda: pack(2, 1, 1))
    node_spectra(2, 0, k2a)
    loads[5].wait()
    own_forward(region0, along_x)
    operator(0)
    cross.wait_recv()
    corner.start()
    pl.when(last_y)(lambda: pack(1, 0, 0))
    pl.when(jnp.logical_not(last_y))(lambda: pack(1, 0, 2))
    node_spectra(1, 2, k2b)
    corner.wait_recv()
    for edge_x in (False, True):
        for edge_y in (False, True):
            here = (last_x if edge_x else jnp.logical_not(last_x),
                    last_y if edge_y else jnp.logical_not(last_y))
            source = (0 if edge_y else 2) if edge_x else (1 if edge_y else 3)
            pl.when(jnp.logical_and(*here))(lambda: pack(1, 0, source))
    node_spectra(1, 3, k2c, lambda: relay(along_y, relayed, 0))
    operator(1)
    places = [(k2a, 2, 0), (k2a, 2, 1), (k2b, 1, 0), (k2c, 1, 0)]
    blend_kernels(half, count_x, count_y, places, kb)
    halo_forward(region0, along_y, relayed, False)
    add_halo(half, count_x, count_y, pitch, c, kb, u)
    finish(0)
    for sweep_index in range(1, ITERS):
        region = regions[sweep_index]
        along_y, along_x, relayed = links[sweep_index]
        own_depth(region)
        own_forward(region, along_x, [relayed[0][0], relayed[1][0]])
        operator(0, 1)
        halo_forward(region, along_y, relayed, True)
        add_halo(half, count_x, count_y, pitch, c, kb, u)
        finish(sweep_index)
    for link in started:
        link.wait_send()


def local(data, precond, psf):
    count_x, count_y, depth = data.shape
    width = psf.shape[2]
    half = width // 2
    region_x, region_y = count_x + 2 * half, count_y + 2 * half
    field, kernel, back = tables(depth, width)
    back = back / (region_x * region_y)
    f32 = jnp.float32
    up = lambda n, m: -(-n // m) * m
    high, columns = up(width, SUB), up(width, LANES // width) // (LANES // width)
    rows, single = rows_of(2, width), rows_of(1, width)
    terms = len(halo_terms(half, count_y))
    pitch = max(region_x, region_y) + SUB
    vmem = lambda *shape: pltpu.VMEM(shape, f32)
    table = lambda *shape: pltpu.VMEM(shape, jnp.bfloat16)
    square = region_x * region_y
    flat = psf.transpose(0, 2, 3, 1, 4).reshape(width, width, 1, width)
    operands = (data, precond, flat, stacked(field), stacked(kernel), stacked(back))
    model, residual = pl.pallas_call(
        functools.partial(whole_kernel, count_x, count_y, half, pitch),
        out_shape=[jax.ShapeDtypeStruct(data.shape, f32)] * 2,
        in_specs=[pl.BlockSpec(memory_space=pltpu.HBM)] * 6,
        out_specs=[pl.BlockSpec(memory_space=pltpu.VMEM)] * 2,
        scratch_shapes=[
            vmem(*data.shape),
            vmem(*data.shape),
            vmem(width, width, width),
            table(*operands[3].shape),
            table(*operands[4].shape),
            table(*operands[5].shape),
            vmem(region_x, region_y, depth),
            vmem(region_x, region_y, depth),
            vmem(width, high, LANES),
            vmem(4, columns, high, LANES),
            vmem(columns, rows, LANES),
            vmem(width * rows, LANES),
            vmem(4, 2, square, LANES),
            vmem(2, width * rows, LANES),
            vmem(2, region_x * rows, LANES),
            vmem(2, region_x * single, LANES),
            vmem(2, region_x * single, LANES),
            vmem(2, region_x // SUB, terms, 2, SUB, LANES),
            vmem(2, square, LANES),
            vmem(2, region_x * pitch, LANES),
            vmem(region_x // SUB, 2, region_y, SUB, LANES),
            vmem(2, 2, count_y * pitch, LANES),
            vmem(count_y // SUB, count_x * SUB, 2 * LANES),
            vmem(2, 2, max(region_x, region_y), SUB, LANES),
            pltpu.SemaphoreType.DMA((6,)),
            pltpu.SemaphoreType.DMA((3 + LINKS * ITERS,)),
            pltpu.SemaphoreType.DMA((3 + LINKS * ITERS,)),
        ],
        compiler_params=pltpu.CompilerParams(
            vmem_limit_bytes=54976 << 10, collective_id=0, has_side_effects=True
        ),
        name="whole",
    )(*operands)
    def tail(a, b, c, e, sems):
        copies = [pltpu.make_async_copy(a, c, sems.at[0]), pltpu.make_async_copy(b, e, sems.at[1])]
        for copy in copies:
            copy.start()
        for copy in copies:
            copy.wait()

    return pl.pallas_call(
        tail,
        out_shape=[jax.ShapeDtypeStruct(data.shape, f32)] * 2,
        in_specs=[pl.BlockSpec(memory_space=pltpu.VMEM)] * 2,
        out_specs=[pl.BlockSpec(memory_space=pl.ANY)] * 2,
        scratch_shapes=[pltpu.SemaphoreType.DMA((2,))],
        compiler_params=pltpu.CompilerParams(vmem_limit_bytes=54976 << 10),
        name="tail",
    )(model, residual)


def solution(mesh):
    placed = (P("gx", "gy", None), P("gx", "gy", None), P("gx", "gy", None, None, None))
    return jax.shard_map(
        local,
        mesh=mesh,
        in_specs=placed,
        out_specs=(P("gx", "gy", None), P("gx", "gy", None)),
        check_vma=False,
    )
```
